32 devices in a mesh: grp: 4 (over z), dev: 8 (over y, x, core).
Axes of the slice: x: 2, y: 2, z: 4, core: 2. Of those that a mesh axis runs over, the one named last changes fastest.
Arguments:
- atm_state: float32 [4, 8, 128, 1024], P('grp', 'dev'), may hold values from -6 to 6
- atm_nbrs: int32 [4, 8, 4, 1024], P('grp', 'dev'), may hold values from 0 to 1279
- atm_send: int32 [4, 8, 256], P('grp', 'dev'), may hold values from 0 to 1023
- atm_mix: float32 [4, 8, 1024], P('grp', 'dev'), may hold values from 0.2 to 0.6
- flux_weight: float32 [24, 128], replicated, may hold values from -0.5 to 0.5
- margin_counts: int32 [4, 8, 1024], P('grp', 'dev'), may hold values from 1 to 4, 1536 in all within a row
- margin_weight: float32 [4, 8, 1536], P('grp', 'dev'), may hold values from 0.05 to 1
- block_owner: int32 [4, 8, 12, 1], P('grp', 'dev'), may hold values from 0 to 1, as said below
- recv_cols: int32 [4, 8, 2, 12, 128], P('grp', 'dev'), may hold values from 0 to 2047
- ocn_state: float32 [4, 8, 80, 2048], P('grp', 'dev'), may hold values from -6 to 6
- ocn_nbrs: int32 [4, 8, 6, 2048], P('grp', 'dev'), may hold values from 0 to 2303
- ocn_send: int32 [4, 8, 256], P('grp', 'dev'), may hold values from 0 to 2047
- ocn_mix: float32 [4, 8, 2048], P('grp', 'dev'), may hold values from 0.1 to 0.4
- force_weight: float32 [80, 24], replicated, may hold values from -1.25 to 1.25
- ret_weight: float32 [12, 80], replicated, may hold values from -0.625 to 0.625
Outputs:
- atm_next: float32 [4, 8, 128, 1024], P('grp', 'dev')
- ocn_next: float32 [4, 8, 80, 2048], P('grp', 'dev')
- atm_remapped: float32 [4, 8, 12, 1024], P('grp', 'dev')
The draws below stay inside these ranges and needn't reach their ends.
Inputs may be any that keep to these rules, and one draw needn't show every extreme that they name: `margin_counts`: the 1024 counts of one partition sum to 1536, and one of them equals 4. `block_owner`: no partition sends more than 12 of its 12 blocks to one ocean group, and every partition sends exactly 12 blocks to one of them.
All inputs are finite; a program needn't handle non-finite values.
Results may differ from the reference program's by a relative error of at most 0.0029.
Values may be sent and summed in bfloat16 or wider, within the bound.
A program may use at most 64 MiB of HBM per device.

```python
import math
import jax
import jax.numpy as jnp
import numpy as np
from jax import lax

LEV_A = 128
LEV_O = 80
FLUX = 24
RET = 12
KA = 4
KO = 6
BLOCK = 128
HS = 128
COLS = 1024
CELLS = 2048
ROWS = 1536
NB = 12
ATM_GRPS = 2
OCN_GRPS = 2
CAP = 12
N_GRP = 4
N_DEV = 8


def draw_block_owner(key, part):
    first_key, second_key = jax.random.split(jax.random.fold_in(key, 7311))
    partitions = N_GRP * N_DEV
    orders = jax.vmap(lambda k: jax.random.permutation(k, OCN_GRPS))(jax.random.split(first_key, partitions))
    listed = jnp.repeat(orders, CAP, axis=1)[:, :NB]
    shuffled = jax.vmap(lambda k, row: jax.random.permutation(k, row))(jax.random.split(second_key, partitions), listed)
    return shuffled.reshape(N_GRP, N_DEV, NB, 1).astype(jnp.int32)


def with_ends(array, key, least, top_value):
    spot = [jax.random.randint(jax.random.fold_in(key, axis), (), 0, length) for axis, length in enumerate(array.shape)]
    widest = array.shape.index(max(array.shape))
    next_to = spot[:widest] + [(spot[widest] + 1) % array.shape[widest]] + spot[widest + 1:]
    return array.at[tuple(spot)].set(least).at[tuple(next_to)].set(top_value)


def block_scale(own_key, dims, pieces, low, largest):
    factor_of = 1.0
    for position, parts in pieces:
        draws = jax.random.uniform(jax.random.fold_in(jax.random.fold_in(own_key, 6), position), (parts,), jnp.float32, low / len(pieces), largest / len(pieces))
        factor_of = factor_of * jnp.repeat(jnp.exp(draws), dims[position] // parts).reshape((-1,) + (1,) * (len(dims) - 1 - position))
    return factor_of


def length_profile(amount, total, most, slope):
    weights = [(1 << 20) // math.isqrt(standing ** slope) + 1 for standing in range(2, amount + 1)]
    spare, given = total - most - (amount - 1), [1] * (amount - 1)
    while spare > 0:
        candidates = [i for i in range(amount - 1) if given[i] < most]
        whole, left = sum([weights[i] for i in candidates]), spare
        for i in candidates:
            addition = min(most - given[i], max(1, left * weights[i] // whole), spare)
            given[i] = given[i] + addition
            spare = spare - addition
    return np.array([most] + given)


def ragged(stream_key, number_of, total, reach, skew):
    if number_of == 2:
        one = jax.random.randint(stream_key, (), max(1, total - reach), min(reach, total - 1) + 1)
        return jnp.stack([one, total - one])
    sizes = jnp.asarray(length_profile(number_of, total, reach, skew), jnp.int32)
    couples = (number_of - 1) // 2
    source_of, sink = sizes[1:1 + 2 * couples:2], sizes[2:2 + 2 * couples:2]
    slack = jnp.minimum(source_of - 1, reach - sink)
    passed = jax.random.randint(jax.random.fold_in(stream_key, 1), (couples,), 0, 1 << 20) % (slack + 1)
    sizes = sizes.at[1:1 + 2 * couples:2].set(source_of - passed).at[2:2 + 2 * couples:2].set(sink + passed)
    return sizes[jax.random.permutation(jax.random.fold_in(stream_key, 2), number_of)]


def bell_draw(rng, dims, deviation, most, pieces=(), held_as=jnp.bfloat16):
    drawn = deviation * jax.random.normal(rng, dims, jnp.float32)
    if pieces:
        drawn = drawn * block_scale(rng, dims, pieces, -0.22, 0.18)
    return jnp.clip(drawn, -most, most).astype(held_as)


def setup_inputs(seed: int = 0) -> dict:
    key_of = jax.random.split(jax.random.key(seed), 16)
    return {
        "atm_state": bell_draw(key_of[0], (N_GRP, N_DEV, LEV_A, COLS), 1.0, 6.0, ((0, 4), (1, 8)), jnp.float32),
        "atm_nbrs": with_ends(jax.random.randint(key_of[1], (N_GRP, N_DEV, KA, COLS), 0, COLS + 2 * HS), jax.random.fold_in(key_of[1], 1), 0, (COLS + 2 * HS) - 1).astype(jnp.int32),
        "atm_send": with_ends(jax.random.randint(key_of[2], (N_GRP, N_DEV, 2 * HS), 0, COLS), jax.random.fold_in(key_of[2], 1), 0, COLS - 1).astype(jnp.int32),
        "atm_mix": jnp.clip(0.2 + 0.400000021 * jax.random.uniform(key_of[3], (N_GRP, N_DEV, COLS), jnp.float32) ** block_scale(key_of[3], (N_GRP, N_DEV, COLS), ((0, 4), (1, 8)), -0.2, 0.2), 0.2, 0.6),
        "flux_weight": bell_draw(key_of[4], (FLUX, LEV_A), LEV_A ** -0.5, 0.5, (), jnp.float32),
        "margin_counts": jax.vmap(lambda own: ragged(own, COLS, ROWS, 4, 1))(jax.random.split(key_of[5], N_GRP * N_DEV)).reshape((N_GRP, N_DEV, COLS)).astype(jnp.int32),
        "margin_weight": jnp.clip(jnp.exp(math.log(1.0) - 2.9957323 * jax.random.uniform(key_of[6], (N_GRP, N_DEV, ROWS), jnp.float32) ** block_scale(key_of[6], (N_GRP, N_DEV, ROWS), ((0, 4), (1, 8)), -0.2, 0.2)), 0.05, 1.0),
        "block_owner": draw_block_owner(jax.random.fold_in(key_of[15], 71), 0),
        "recv_cols": with_ends(jax.random.randint(key_of[8], (N_GRP, N_DEV, ATM_GRPS, CAP, BLOCK), 0, CELLS), jax.random.fold_in(key_of[8], 1), 0, CELLS - 1).astype(jnp.int32),
        "ocn_state": bell_draw(key_of[9], (N_GRP, N_DEV, LEV_O, CELLS), 1.0, 6.0, ((0, 4), (1, 8)), jnp.float32),
        "ocn_nbrs": with_ends(jax.random.randint(key_of[10], (N_GRP, N_DEV, KO, CELLS), 0, CELLS + 2 * HS), jax.random.fold_in(key_of[10], 1), 0, (CELLS + 2 * HS) - 1).astype(jnp.int32),
        "ocn_send": with_ends(jax.random.randint(key_of[11], (N_GRP, N_DEV, 2 * HS), 0, CELLS), jax.random.fold_in(key_of[11], 1), 0, CELLS - 1).astype(jnp.int32),
        "ocn_mix": jnp.clip(0.1 + 0.3 * jax.random.uniform(key_of[12], (N_GRP, N_DEV, CELLS), jnp.float32) ** block_scale(key_of[12], (N_GRP, N_DEV, CELLS), ((0, 4), (1, 8)), -0.2, 0.2), 0.1, 0.4),
        "force_weight": bell_draw(key_of[13], (LEV_O, FLUX), FLUX ** -0.5, 1.25, (), jnp.float32),
        "ret_weight": bell_draw(key_of[14], (RET, LEV_O), LEV_O ** -0.5, 0.625, (), jnp.float32),
    }


EXACT_DOT = lax.Precision.HIGHEST


def stencil(state, pool, neighbours, mixing):
    total = jnp.take(pool, neighbours[0], axis=1)
    for which in range(1, neighbours.shape[0]):
        total = total + jnp.take(pool, neighbours[which], axis=1)
    return state + mixing[None, :] * (total / neighbours.shape[0] - state)


def pick_columns(values, indices):
    return jnp.take(values, indices, axis=1)


def pooled(state, send_list):
    half = send_list.shape[-1] // 2
    packed = jax.vmap(jax.vmap(pick_columns))(state, send_list)
    from_lower = jnp.roll(packed[..., half:], 1, axis=1)
    from_upper = jnp.roll(packed[..., :half], -1, axis=1)
    return jnp.concatenate([state, from_lower, from_upper], axis=3)


def column_ids(counts):
    return jnp.repeat(jnp.arange(COLS, dtype=jnp.int32), counts, total_repeat_length=ROWS)


def block_slots(owner):
    order = jnp.arange(owner.shape[0], dtype=jnp.int32)
    earlier = (owner[None, :] == owner[:, None]) & (order[None, :] < order[:, None])
    return jnp.sum(earlier.astype(jnp.int32), axis=1)


def remap_back(values, weights, column):
    weighted = jax.ops.segment_sum(values * weights[:, None], column, num_segments=COLS)
    weight_sum = jax.ops.segment_sum(weights, column, num_segments=COLS)
    return (weighted / weight_sum[:, None]).T


def reference(atm_state, atm_nbrs, atm_send, atm_mix, flux_weight, margin_counts, margin_weight, block_owner, recv_cols, ocn_state, ocn_nbrs, ocn_send, ocn_mix, force_weight, ret_weight):
    groups = atm_state.shape[0]
    devices = atm_state.shape[1]
    atm_groups = groups // 2
    sweep = jax.vmap(jax.vmap(stencil))
    air = atm_state[:atm_groups]
    air_next = sweep(air, pooled(air, atm_send[:atm_groups]), atm_nbrs[:atm_groups], atm_mix[:atm_groups])
    atm_next = jnp.concatenate([air_next, atm_state[atm_groups:]], axis=0)
    sea = ocn_state[atm_groups:]
    sea_base = sweep(sea, pooled(sea, ocn_send[atm_groups:]), ocn_nbrs[atm_groups:], ocn_mix[atm_groups:])
    fluxes = jnp.einsum("fl,gdlc->gdfc", flux_weight, air_next, precision=EXACT_DOT)
    column = jax.vmap(jax.vmap(column_ids))(margin_counts[:atm_groups])
    weights = margin_weight[:atm_groups]
    row_values = (jax.vmap(jax.vmap(pick_columns))(fluxes, column) * weights[:, :, None, :]).astype(jnp.bfloat16)
    owner = block_owner[:atm_groups, :, :, 0]
    slot = jax.vmap(jax.vmap(block_slots))(owner)
    sender = jnp.arange(atm_groups, dtype=jnp.int32)[:, None, None]
    partition = jnp.arange(devices, dtype=jnp.int32)[None, :, None]
    cell = recv_cols[atm_groups + owner, partition, sender, slot]
    target = ((owner * devices + partition)[..., None] * CELLS + cell).reshape(-1)
    flat_rows = row_values.reshape(atm_groups, devices, FLUX, NB, BLOCK).transpose(0, 1, 3, 4, 2).reshape(-1, FLUX).astype(jnp.float32)
    cell_flux = jnp.zeros((OCN_GRPS * devices * CELLS, FLUX), jnp.float32).at[target].add(flat_rows)
    cell_flux = cell_flux.reshape(OCN_GRPS, devices, CELLS, FLUX)
    forcing = jnp.einsum("lf,odcf->odlc", force_weight, cell_flux, precision=EXACT_DOT)
    ocn_next = jnp.concatenate([ocn_state[:atm_groups], sea_base + forcing], axis=0)
    returned = jnp.einsum("rl,odlc->odcr", ret_weight, sea, precision=EXACT_DOT).astype(jnp.bfloat16)
    looked = returned.reshape(-1, RET)[target].astype(jnp.float32).reshape(atm_groups, devices, ROWS, RET)
    remapped = jax.vmap(jax.vmap(remap_back))(looked, weights, column)
    remapped = jnp.concatenate([remapped, jnp.zeros((groups - atm_groups, devices, RET, COLS), jnp.float32)], axis=0)
    return atm_next, ocn_next, remapped
```

```python
import functools

import jax
import jax.numpy as jnp
from jax import lax
from jax.experimental import pallas as pl
from jax.experimental.pallas import tpu as pltpu
from jax.sharding import PartitionSpec as P

EXACT = lax.Precision.HIGHEST
BF = jnp.bfloat16
F32 = jnp.float32
I32 = jnp.int32
NT = (((1,), (1,)), ((), ()))
TN = (((0,), (0,)), ((), ()))


def mm(a, b):
    return jnp.dot(a, b, preferred_element_type=F32)


def two_parts(x):
    rest = x - x.astype(BF).astype(F32)
    return jnp.concatenate([x, rest], axis=0).astype(BF)


def joined(x):
    half = x.shape[0] // 2
    return x[:half] + x[half:]


def low_hot(low, t):
    place = lax.broadcasted_iota(I32, low.shape, 0).astype(F32).astype(BF)
    return jnp.where(low - jnp.asarray(16.0 * t, BF) == place, jnp.asarray(1, BF), jnp.asarray(0, BF))


def as_rows(idx, rows):
    return jnp.broadcast_to(idx.astype(F32), (rows, idx.shape[1])).astype(BF)


def hot_rows(high, h, rows):
    return jnp.where(jnp.broadcast_to(high, (rows, high.shape[1])) == h, 1.0, 0.0).astype(BF)


def one_hot(idx, rows, base):
    width = idx.shape[1]
    place = lax.broadcasted_iota(I32, (rows, width), 0) + base
    return jnp.where(place == idx, 1.0, 0.0).astype(BF)


def counts_matrix(out_ref, high_ref, idx_rows, base, at):
    width = idx_rows[0].shape[1]
    highs = out_ref.shape[0] // base
    bits = base.bit_length() - 1
    low = [as_rows(i & (base - 1), 16) for i in idx_rows]
    for k, i in enumerate(idx_rows):
        for h in range(highs):
            high_ref[k * highs + h, :, :width] = hot_rows(i >> bits, h, 16)
    for t in range(base // 16):
        parts = [low_hot(i, t) for i in low]
        for h in range(highs):
            total = parts[0] * high_ref[h, :, :width]
            for k in range(1, len(parts)):
                total = total + parts[k] * high_ref[k * highs + h, :, :width]
            out_ref[pl.ds(h * base + t * 16, 16), at] = total


def base_of(length):
    return 256 if length % 256 == 0 else 128


def row_columns(counts, rows):
    lines = counts.shape[0]
    wide = jnp.concatenate([counts.astype(F32), jnp.zeros((-lines % 16, 128), F32)], axis=0).astype(BF)
    lines = wide.shape[0]
    i = lax.broadcasted_iota(I32, (128, 128), 0)
    j = lax.broadcasted_iota(I32, (128, 128), 1)
    within = mm(wide, jnp.where(i <= j, 1.0, 0.0).astype(BF))
    i = lax.broadcasted_iota(I32, (lines, lines), 0)
    j = lax.broadcasted_iota(I32, (lines, lines), 1)
    ones = jnp.ones((128, 128), BF)
    before = mm(mm(jnp.where(j < i, 1.0, 0.0).astype(BF), wide).astype(BF), ones)
    upto = mm(mm(jnp.where(j <= i, 1.0, 0.0).astype(BF), wide).astype(BF), ones)
    offsets = within + before
    high = jnp.floor(offsets * (1.0 / 256.0)) * 256.0
    halves = jnp.concatenate([high, offsets - high], axis=0).astype(BF)
    tiles = rows // 128
    at = lax.broadcasted_iota(I32, (lines, rows), 1).astype(F32)
    ends = jnp.concatenate([upto] * tiles, axis=1)
    starts = jnp.concatenate([before] * tiles, axis=1)
    passed = jnp.where(ends <= at, 1.0, 0.0)
    line = jnp.where(starts <= at, 1.0, 0.0) - passed
    line = jnp.concatenate([line, line], axis=0).astype(BF)
    ends_in = lax.dot_general(halves, line, TN, preferred_element_type=F32)
    at = lax.broadcasted_iota(I32, (128, rows), 1).astype(F32)
    inner = jnp.sum(jnp.where(ends_in <= at, 1.0, 0.0), axis=0, keepdims=True)
    return 128.0 * jnp.sum(passed, axis=0, keepdims=True) + inner


def kernel(
    sizes,
    air_hbm, anbr_hbm, asend_hbm, amix_hbm, fw_hbm, counts_hbm, mw_hbm, owner_hbm,
    recv_hbm, sea_hbm, onbr_hbm, osend_hbm, omix_hbm, force_hbm, retw_hbm,
    air_out, sea_out, back_out,
    anbr, asend, amix, fw, counts, mw, owner, recv, onbr, osend, omix, force, retw_in,
    pack, halo, apool, gpool, opool, amat, omat0, omat1, member, lowmat, lowrow, spread, high, high1,
    codes_out, codes_in, up_out, up_in, down_out, down_in, retw, slab, ret_bf, wide_force,
    load, halo_send, halo_recv, code_send, code_recv, up_send, relay_send, up_recv, down_send, down_recv,
):
    groups, devs, air_groups = sizes
    sea_groups = groups - air_groups
    g, d = lax.axis_index("grp"), lax.axis_index("dev")
    lower, upper = lax.rem(d + devs - 1, devs), lax.rem(d + 1, devs)
    is_air = g < air_groups
    mine = jnp.where(is_air, g, g - air_groups)
    half = halo.shape[2]
    capacity, block = recv.shape[2], recv.shape[4]
    span = capacity * block
    levels_a, columns = air_out.shape[2:]
    levels_o, cells = sea_out.shape[2:]
    fields = fw.shape[0]
    ret_fields = retw_in.shape[0]
    ret_pad = retw.shape[0]
    blocks = owner.shape[3]
    row_count = mw.shape[2]
    pairs = blocks // 2
    same = capacity == blocks
    base = lowmat.shape[0]
    bits = base.bit_length() - 1
    highs = cells // base
    field_pad = spread.shape[0] // highs
    width = high.shape[2]

    barrier = pltpu.get_barrier_semaphore()
    pl.semaphore_signal(barrier, inc=1, device_id={"dev": lower})
    pl.semaphore_signal(barrier, inc=1, device_id={"dev": upper})

    loads = [
        pltpu.make_async_copy(a, b, load.at[i])
        for i, (a, b) in enumerate((
            (air_hbm, air_out), (anbr_hbm, anbr), (asend_hbm, asend), (amix_hbm, amix), (fw_hbm, fw),
            (counts_hbm, counts), (mw_hbm, mw), (owner_hbm, owner), (recv_hbm, recv), (sea_hbm, sea_out),
            (onbr_hbm, onbr), (osend_hbm, osend), (omix_hbm, omix), (force_hbm, force), (retw_hbm, retw_in),
        ))
    ]
    (l_air, l_anbr, l_asend, l_amix, l_fw, l_counts, l_mw, l_owner,
     l_recv, l_sea, l_onbr, l_osend, l_omix, l_force, l_retw) = loads

    def halos(levels):
        return [
            pltpu.make_async_remote_copy(
                src_ref=pack.at[1 - side, :levels], dst_ref=halo.at[side, :levels],
                send_sem=halo_send.at[side], recv_sem=halo_recv.at[side],
                device_id={"dev": upper if side == 0 else lower})
            for side in range(2)
        ]

    def code_copy(s, o):
        return pltpu.make_async_remote_copy(
            src_ref=codes_out, dst_ref=codes_in.at[s], send_sem=code_send.at[o],
            recv_sem=code_recv.at[s], device_id={"grp": air_groups + o})

    def up_copy(s, p):
        return pltpu.make_async_remote_copy(
            src_ref=up_out.at[p], dst_ref=up_in.at[s, p], send_sem=up_send.at[p],
            recv_sem=up_recv.at[s, p], device_id={"grp": air_groups})

    def relay_copy(s, p):
        return pltpu.make_async_remote_copy(
            src_ref=up_in.at[s, p], dst_ref=up_in.at[s, p], send_sem=relay_send.at[s, p],
            recv_sem=up_recv.at[s, p], device_id={"grp": g + 1})

    def down_copy(s, o):
        return pltpu.make_async_remote_copy(
            src_ref=down_out.at[s], dst_ref=down_in.at[o], send_sem=down_send.at[s],
            recv_sem=down_recv.at[o], device_id={"grp": s})

    def packed(state_ref, send_ref, pool):
        levels, length = state_ref.shape[2:]
        top = state_ref[0, 0].astype(BF)
        pool[:, :length] = top
        chosen = mm(top, one_hot(send_ref[0], length, 0)).astype(BF)
        pack[0, :levels, :] = chosen[:, :half]
        pack[1, :levels, :] = chosen[:, half:]

    def take_halo(copies, pool, levels, length):
        for c in copies:
            c.wait()
        for side in range(2):
            at = slice(length + side * half, length + (side + 1) * half)
            pool[:, at] = halo[side, :levels, :]

    @pl.when(is_air)
    def _():
        for o in range(sea_groups):
            pl.semaphore_signal(barrier, inc=1, device_id={"grp": air_groups + o})
        for c in (l_asend, l_air, l_owner, l_counts, l_anbr, l_fw, l_amix, l_mw, l_sea):
            c.start()
        neighbours = anbr.shape[2]
        excess = row_count - columns
        tile = 256

        l_asend.wait()
        l_air.wait()
        packed(air_out, asend, apool)
        l_owner.wait()
        owners = [owner[0, 0, 0, b] for b in range(blocks)]
        slots = []
        for b in range(blocks):
            s = jnp.int32(b if same else 0)
            if not same:
                for e in range(b):
                    s = s + jnp.where(owners[e] == owners[b], 1, 0)
            slots.append(s)
        for b in range(blocks):
            codes_out[b : b + 1, :] = jnp.full((1, 128), owners[b] * capacity + slots[b], I32)
        if codes_out.shape[0] > blocks:
            codes_out[blocks:, :] = jnp.full((codes_out.shape[0] - blocks, 128), -1, I32)
        pl.semaphore_wait(barrier, 2 + sea_groups)
        sides = halos(levels_a)
        for c in sides:
            c.start()
        for o in range(sea_groups):
            code_copy(mine, o).start()

        l_counts.wait()
        column = row_columns(counts[...], row_count).astype(I32)
        low, high_of = column & (tile - 1), column >> (tile.bit_length() - 1)
        low_rows = as_rows(low, 16)

        def reach(p):
            first = max(0, p * tile - excess) // tile
            last = min(columns - 1, p * tile + tile - 1) // tile
            return range(first, last + 1)

        for p in range(row_count // tile):
            at = slice(p * tile, (p + 1) * tile)
            marks = [hot_rows(high_of[:, at], h, 16) for h in reach(p)]
            for t in range(tile // 16):
                part = low_hot(low_rows[:, at], t)
                for i, h in enumerate(reach(p)):
                    member[h * tile + t * 16 : h * tile + (t + 1) * 16, at] = part * marks[i]

        l_anbr.wait()
        base_a = base_of(amat.shape[0])

        def build(c, _):
            at = pl.ds(pl.multiple_of(c * width, width), width)
            rows_in = [anbr[0, 0, k : k + 1, at] for k in range(neighbours)]
            counts_matrix(amat, high, rows_in, base_a, at)
            return _

        lax.fori_loop(0, columns // width, build, 0)

        l_fw.wait()
        state = air_out[0, 0]
        top = state.astype(BF)
        weight = two_parts(fw[...])
        own = joined(mm(weight, top) + mm(weight, (state - top.astype(F32)).astype(BF)))
        gpool[:, :columns] = two_parts(own)
        take_halo(sides, apool, levels_a, columns)
        gpool[:, columns:] = two_parts(joined(mm(weight, apool[:, columns:])))
        l_amix.wait()
        l_mw.wait()
        for c in range(columns // tile):
            at = slice(c * tile, (c + 1) * tile)
            mean = joined(mm(gpool[...], amat[:, at])) * (1.0 / neighbours)
            here = own[:, at]
            slab[: 2 * fields, at] = two_parts(here + amix[0, :, at] * (mean - here))
        for p in range(row_count // tile):
            at = slice(p * tile, (p + 1) * tile)
            ks = reach(p)
            ks = slice(ks[0] * tile, (ks[-1] + 1) * tile)
            values = joined(mm(slab[: 2 * fields, ks], member[ks, at])) * mw[0, :, at]
            per = tile // block
            for q in range(per // 2):
                b = slice(2 * q * block, (2 * q + 1) * block), slice((2 * q + 1) * block, (2 * q + 2) * block)
                up_out[p * (per // 2) + q] = jnp.concatenate([values[:, b[0]], values[:, b[1]]], axis=0).astype(BF)
                up_copy(mine, p * (per // 2) + q).start()
        for c in range(columns // width):
            at = slice(c * width, (c + 1) * width)
            mean = mm(apool[...], amat[:, at]) * (1.0 / neighbours)
            here = air_out[0, 0, :, at]
            air_out[0, 0, :, at] = here + amix[0, :, at] * (mean - here)
        for o in range(sea_groups):
            down_copy(0, o).wait_recv()
        for b in range(blocks):
            at = slice(b * block, (b + 1) * block)
            share = jnp.broadcast_to(mw[0, :, at], (ret_pad, block))
            value = down_in[owners[b], slots[b]].astype(F32) * share
            slab[: 2 * ret_pad, at] = two_parts(value)
            slab[2 * ret_pad : 4 * ret_pad, at] = two_parts(share)
        for c in range(columns // tile):
            at = slice(c * tile, (c + 1) * tile)
            rs = slice(c * tile, min(row_count, (c + 1) * tile + excess))
            sums = lax.dot_general(slab[: 4 * ret_pad, rs], member[at, rs], NT, preferred_element_type=F32)
            ratio = joined(sums[: 2 * ret_pad]) / joined(sums[2 * ret_pad :])
            for f in range(ret_fields):
                back_out[0, f, :, at] = ratio[f : f + 1]
        for o in range(sea_groups):
            code_copy(mine, o).wait_send()
        for p in range(pairs):
            up_copy(mine, p).wait_send()
        l_sea.wait()

    @pl.when(jnp.logical_not(is_air))
    def _():
        for s in range(air_groups):
            pl.semaphore_signal(barrier, inc=1, device_id={"grp": s})
        not_first, not_last = mine > 0, mine < sea_groups - 1

        @pl.when(not_first)
        def _():
            pl.semaphore_signal(barrier, inc=1, device_id={"grp": g - 1})

        @pl.when(not_last)
        def _():
            pl.semaphore_signal(barrier, inc=1, device_id={"grp": g + 1})

        for c in (l_osend, l_sea, l_recv, l_retw, l_onbr, l_omix, l_force, l_air):
            c.start()
        l_osend.wait()
        l_sea.wait()
        packed(sea_out, osend, opool)
        links = jnp.where(not_first, 1, 0) + jnp.where(not_last, 1, 0)
        pl.semaphore_wait(barrier, 2 + air_groups + links)
        sides = halos(levels_o)
        for c in sides:
            c.start()
        neighbours = onbr.shape[1]
        l_retw.wait()
        retw[...] = jnp.zeros(retw.shape, F32)
        retw[:ret_fields] = retw_in[...]
        returned = jnp.dot(
            retw[...], sea_out[0, 0], precision=EXACT, preferred_element_type=F32).astype(BF)
        for h in range(highs):
            ret_bf[h * ret_pad : (h + 1) * ret_pad] = returned[:, h * base : (h + 1) * base]
        l_recv.wait()

        def slot_ids(s):
            return jnp.concatenate([recv[0, 0, k, s : s + 1, :] for k in range(capacity)], axis=1)

        for s in range(air_groups):
            idx = slot_ids(s)
            at = slice(s * span, (s + 1) * span)
            low = as_rows(idx & (base - 1), 16)
            for t in range(base // 16):
                lowmat[t * 16 : (t + 1) * 16, at] = low_hot(low, t)
            found = mm(ret_bf[...], lowmat[:, at])
            high_of = jnp.broadcast_to(idx >> bits, (ret_pad, span))
            looked = jnp.zeros((ret_pad, span), F32)
            for h in range(highs):
                looked = jnp.where(high_of == h, found[h * ret_pad : (h + 1) * ret_pad], looked)
            for k in range(capacity):
                down_out[s, k] = looked[:, k * block : (k + 1) * block].astype(BF)
            down_copy(s, mine).start()
        spread[...] = jnp.zeros(spread.shape, BF)
        wide_force[...] = jnp.zeros(wide_force.shape, F32)
        l_force.wait()
        strong = force[...]
        wide_force[:fields, :levels_o] = strong
        wide_force[field_pad : field_pad + fields, :levels_o] = strong
        wide_force[2 * field_pad : 2 * field_pad + fields, :levels_o] = strong - strong.astype(BF).astype(F32)
        force_rows = wide_force[...].T[:levels_o, : 3 * field_pad].astype(BF)
        l_onbr.wait()
        l_omix.wait()
        base_p = base_of(omat0.shape[0])
        tiles = cells // width

        def build(c, mat, marks):
            at = pl.ds(pl.multiple_of(c * width, width), width)
            rows_in = [onbr[0, k, :, at] for k in range(neighbours)]
            counts_matrix(mat, marks, rows_in, base_p, slice(0, width))

        def product(c, mat):
            at = pl.ds(pl.multiple_of(c * width, width), width)
            mean = mm(opool[...], mat[...]) * (1.0 / neighbours)
            here = sea_out[0, 0, :, at]
            sea_out[0, 0, :, at] = here + omix[0, :, at] * (mean - here)

        build(0, omat0, high)
        take_halo(sides, opool, levels_o, cells)

        def pair(i, _):
            product(2 * i, omat0)
            build(2 * i + 1, omat1, high1)
            product(2 * i + 1, omat1)
            build(2 * i + 2, omat0, high)
            return _

        lax.fori_loop(0, tiles // 2 - 1, pair, 0)
        product(tiles - 2, omat0)
        build(tiles - 1, omat1, high1)
        product(tiles - 1, omat1)
        row_span = blocks * block
        rows_low, rows_high = [], []
        for s in range(air_groups):
            code_copy(s, 0).wait_recv()
            place = codes_in[s] - mine * capacity
            ids = []
            for b in range(blocks):
                here = place[b : b + 1]
                held = (here >= 0) & (here < capacity)
                if same:
                    cell = recv[0, 0, b, s : s + 1, :]
                else:
                    cell = jnp.zeros((1, block), I32)
                    for k in range(capacity):
                        cell = jnp.where(here == k, recv[0, 0, k, s : s + 1, :], cell)
                ids.append(jnp.where(held, cell, -1))
            rows_high.append([i >> bits for i in ids])
            if not same:
                low = as_rows(jnp.concatenate(ids, axis=1) & (base - 1), 16)
                for t in range(base // 16):
                    lowrow[t * 16 : (t + 1) * 16, s * row_span : (s + 1) * row_span] = low_hot(low, t)
        near = lowmat if same else lowrow
        flux = jnp.zeros((highs * field_pad, base), F32)
        for p in range(pairs):
            for s in range(air_groups):
                relay_copy(s, p).wait_recv()

                @pl.when(not_last)
                def _():
                    relay_copy(s, p).start()

            for s in range(air_groups):
                arrived = up_in[s, p].astype(F32)
                for j in range(2):
                    at = slice(s * row_span + (2 * p + j) * block, s * row_span + (2 * p + j + 1) * block)
                    part = arrived[j * fields : (j + 1) * fields]
                    high_of = jnp.broadcast_to(rows_high[s][2 * p + j], (fields, block))
                    for h in range(highs):
                        spread[h * field_pad : h * field_pad + fields, at] = (
                            jnp.where(high_of == h, part, 0.0).astype(BF))
                at = slice(s * row_span + 2 * p * block, s * row_span + (2 * p + 2) * block)
                flux = flux + lax.dot_general(spread[:, at], near[:, at], NT, preferred_element_type=F32)
        for h in range(highs):
            at = slice(h * base, (h + 1) * base)
            here = flux[h * field_pad : (h + 1) * field_pad]
            top = here.astype(BF)
            rest = (here - top.astype(F32)).astype(BF)
            sea_out[0, 0, :, at] += mm(force_rows, jnp.concatenate([top, rest, top], axis=0))
        for s in range(air_groups):
            down_copy(s, mine).wait_send()

        @pl.when(not_last)
        def _():
            for p in range(pairs):
                for s in range(air_groups):
                    relay_copy(s, p).wait_send()

        back_out[...] = jnp.zeros(back_out.shape, F32)
        l_air.wait()


def finish(a, b, c, a_out, b_out, c_out, sem):
    copies = [
        pltpu.make_async_copy(x, y, sem.at[i])
        for i, (x, y) in enumerate(((a, a_out), (b, b_out), (c, c_out)))
    ]
    for x in copies:
        x.start()
    for x in copies:
        x.wait()


def solution(mesh):
    groups, devs = mesh.shape["grp"], mesh.shape["dev"]
    in_specs = (
        P("grp", "dev", None, None), P("grp", "dev", None, None), P("grp", "dev", None),
        P("grp", "dev", None), P(), P("grp", "dev", None), P("grp", "dev", None),
        P("grp", "dev", None, None), P("grp", "dev", None, None, None),
        P("grp", "dev", None, None), P("grp", "dev", None, None), P("grp", "dev", None),
        P("grp", "dev", None), P(), P(),
    )
    out_specs = (P("grp", "dev", None, None),) * 3

    def on_device(*args):
        args = list(args)
        args[5] = args[5].reshape(-1, 128)
        args[7] = args[7].transpose(0, 1, 3, 2)
        args[8] = args[8].transpose(0, 1, 3, 2, 4)
        args[10] = args[10].transpose(0, 2, 1, 3)
        args[13] = args[13].T
        air, anbr, asend, amix, fw, counts, mw, owner, recv, sea, onbr, osend, omix, force, ret = args
        levels_a, columns = air.shape[2:]
        levels_o, cells = sea.shape[2:]
        half = asend.shape[2] // 2
        capacity, air_groups, block = recv.shape[2:]
        sea_groups = groups - air_groups
        blocks = owner.shape[3]
        fields, ret_fields = fw.shape[0], ret.shape[0]
        ret_pad = -(-ret_fields // 16) * 16
        field_pad = -(-fields // 16) * 16
        row_count = mw.shape[2]
        pairs = blocks // 2
        pool_a, pool_o = columns + 2 * half, cells + 2 * half
        width = 256
        base, span = base_of(cells), air_groups * capacity * block
        row_span = air_groups * blocks * block
        same = capacity == blocks
        deep = max(
            anbr.shape[2] * (pool_a // base_of(pool_a)),
            onbr.shape[1] * (pool_o // base_of(pool_o)),
        )
        code_rows = -(-blocks // 8) * 8
        V = pltpu.VMEM
        dma = pltpu.SemaphoreType.DMA
        kept = [V(x.shape, x.dtype) for x in (anbr, asend, amix, fw, counts, mw)]
        kept += [pltpu.SMEM(owner.shape, owner.dtype)]
        kept += [V(x.shape, x.dtype) for x in (recv, onbr, osend, omix, force, ret)]
        scratch = kept + [
            V((2, max(levels_a, levels_o), half), BF), V((2, max(levels_a, levels_o), half), BF),
            V((levels_a, pool_a), BF), V((2 * fields, pool_a), BF), V((levels_o, pool_o), BF),
            V((pool_a, columns), BF), V((pool_o, width), BF), V((pool_o, width), BF),
            V((columns, row_count), BF), V((base, span), BF),
            V((base if not same else 16, row_span if not same else 128), BF),
            V((cells // base * field_pad, row_span), BF),
            V((deep, 16, width), BF), V((deep, 16, width), BF),
            V((code_rows, 128), I32), V((air_groups, code_rows, 128), I32),
            V((pairs, 2 * fields, block), BF), V((air_groups, pairs, 2 * fields, block), BF),
            V((air_groups, capacity, ret_pad, block), BF), V((sea_groups, capacity, ret_pad, block), BF),
            V((ret_pad, levels_o), F32),
            V((max(4 * ret_pad, 2 * fields), max(row_count, columns)), BF),
            V((cells // base * ret_pad, base), BF),
            V((128, 128), F32),
            dma((15,)), dma((2,)), dma((2,)), dma((sea_groups,)), dma((air_groups,)),
            dma((pairs,)), dma((air_groups, pairs)), dma((air_groups, pairs)),
            dma((air_groups,)), dma((sea_groups,)),
        ]
        vmem = pl.BlockSpec(memory_space=pltpu.VMEM)
        outs = (
            jax.ShapeDtypeStruct(air.shape, F32),
            jax.ShapeDtypeStruct(sea.shape, F32),
            jax.ShapeDtypeStruct((1, ret_fields, 1, columns), F32),
        )
        parts = pl.pallas_call(
            functools.partial(kernel, (groups, devs, air_groups)),
            out_shape=outs,
            in_specs=[pl.BlockSpec(memory_space=pltpu.HBM)] * 15,
            out_specs=(vmem,) * 3,
            scratch_shapes=scratch,
            compiler_params=pltpu.CompilerParams(
                collective_id=0, has_side_effects=True, vmem_limit_bytes=48 * 1024 * 1024),
            name="couple",
        )(*[pltpu.with_memory_space_constraint(x, pltpu.HBM) for x in args])
        air_next, sea_next, back = pl.pallas_call(
            finish,
            out_shape=outs,
            in_specs=[pl.BlockSpec(memory_space=pl.ANY)] * 3,
            out_specs=(pl.BlockSpec(memory_space=pl.ANY),) * 3,
            scratch_shapes=[dma((3,))],
            compiler_params=pltpu.CompilerParams(vmem_limit_bytes=1024 * 1024),
            name="finish",
        )(*parts)
        return air_next, sea_next, back.transpose(0, 2, 1, 3)

    return jax.shard_map(
        on_device, mesh=mesh, in_specs=in_specs, out_specs=out_specs, check_vma=False)
```

```python
import functools

import jax
import jax.numpy as jnp
from jax import lax
from jax.experimental import pallas as pl
from jax.experimental.pallas import tpu as pltpu
from jax.sharding import PartitionSpec as P

EXACT = lax.Precision.HIGHEST
BF = jnp.bfloat16
F32 = jnp.float32
I32 = jnp.int32
NT = (((1,), (1,)), ((), ()))
TN = (((0,), (0,)), ((), ()))


def mm(a, b):
    return jnp.dot(a, b, preferred_element_type=F32)


def two_parts(x):
    rest = x - x.astype(BF).astype(F32)
    return jnp.concatenate([x, rest], axis=0).astype(BF)


def joined(x):
    half = x.shape[0] // 2
    return x[:half] + x[half:]


def low_hot(low, t):
    place = lax.broadcasted_iota(I32, low.shape, 0).astype(F32) + 16.0 * t
    return jnp.where(low == place.astype(BF), jnp.asarray(1, BF), jnp.asarray(0, BF))


def as_rows(idx, rows):
    return jnp.broadcast_to(idx.astype(F32), (rows, idx.shape[1])).astype(BF)


def hot_rows(high, h, rows):
    return jnp.where(as_rows(high, rows) == jnp.asarray(h, BF), jnp.asarray(1, BF), jnp.asarray(0, BF))


def one_hot_matrix(out_ref, idx, base):
    bits = base.bit_length() - 1
    low = as_rows(idx & (base - 1), 16)
    marks = [hot_rows(idx >> bits, h, 16) for h in range(out_ref.shape[0] // base)]
    for t in range(base // 16):
        part = low_hot(low, t)
        for h, mark in enumerate(marks):
            out_ref[h * base + t * 16 : h * base + (t + 1) * 16, :] = part * mark


def couples(highs, neighbours):
    step = 2 if neighbours < 8 else 1
    return [tuple(range(h, min(h + step, highs))) for h in range(0, highs, step)]


def scale_at(position, length, base, neighbours):
    for couple in couples(length // base, neighbours):
        if position // base in couple:
            return 16.0 if len(couple) == 2 and position // base == couple[0] else 1.0


def scaled(x, at, length, base, neighbours):
    return x * jnp.asarray(scale_at(at, length, base, neighbours), BF)


def counts_matrix(out_ref, high_ref, idx_rows, base, at):
    highs = out_ref.shape[0] // base
    bits = base.bit_length() - 1
    lines = couples(highs, len(idx_rows))
    low = [as_rows(i & (base - 1), 16) for i in idx_rows]
    for k, i in enumerate(idx_rows):
        top = as_rows(i >> bits, 16)
        for n, couple in enumerate(lines):
            mark = jnp.where(top == jnp.asarray(couple[-1], BF), jnp.asarray(1, BF), jnp.asarray(0, BF))
            if len(couple) == 2:
                mark = jnp.where(top == jnp.asarray(couple[0], BF), jnp.asarray(1 / 16, BF), mark)
            high_ref[k * len(lines) + n] = mark
    for t in range(base // 16):
        parts = [low_hot(i, t) for i in low]
        for n, couple in enumerate(lines):
            total = parts[0] * high_ref[n]
            for k in range(1, len(parts)):
                total = total + parts[k] * high_ref[k * len(lines) + n]
            if len(couple) == 2:
                whole = (total + jnp.asarray(128, BF)) - jnp.asarray(128, BF)
                out_ref[couple[0] * base + t * 16 : couple[0] * base + (t + 1) * 16, at] = total - whole
                total = whole
            out_ref[couple[-1] * base + t * 16 : couple[-1] * base + (t + 1) * 16, at] = total


def base_of(length):
    return 256 if length % 256 == 0 else 128


def row_columns(counts, rows):
    lines = counts.shape[0]
    wide = jnp.concatenate([counts.astype(F32), jnp.zeros((-lines % 16, 128), F32)], axis=0).astype(BF)
    lines = wide.shape[0]
    i = lax.broadcasted_iota(I32, (128, 128), 0)
    j = lax.broadcasted_iota(I32, (128, 128), 1)
    within = mm(wide, jnp.where(i <= j, 1.0, 0.0).astype(BF))
    i = lax.broadcasted_iota(I32, (lines, lines), 0)
    j = lax.broadcasted_iota(I32, (lines, lines), 1)
    ones = jnp.ones((128, 128), BF)
    before = mm(mm(jnp.where(j < i, 1.0, 0.0).astype(BF), wide).astype(BF), ones)
    upto = mm(mm(jnp.where(j <= i, 1.0, 0.0).astype(BF), wide).astype(BF), ones)
    offsets = within + before
    high = jnp.floor(offsets * (1.0 / 256.0)) * 256.0
    halves = jnp.concatenate([high, offsets - high], axis=0).astype(BF)
    tiles = rows // 128
    at = lax.broadcasted_iota(I32, (lines, rows), 1).astype(F32)
    ends = jnp.concatenate([upto] * tiles, axis=1)
    starts = jnp.concatenate([before] * tiles, axis=1)
    passed = jnp.where(ends <= at, 1.0, 0.0)
    line = jnp.where(starts <= at, 1.0, 0.0) - passed
    line = jnp.concatenate([line, line], axis=0).astype(BF)
    ends_in = lax.dot_general(halves, line, TN, preferred_element_type=F32)
    at = lax.broadcasted_iota(I32, (128, rows), 1).astype(F32)
    inner = jnp.sum(jnp.where(ends_in <= at, 1.0, 0.0), axis=0, keepdims=True)
    return 128.0 * jnp.sum(passed, axis=0, keepdims=True) + inner


def kernel(sizes, *refs):
    pl.run_scoped(
        functools.partial(body, sizes[:3], refs),
        *(pltpu.SemaphoreType.DMA(n) for n in sizes[3]))


def body(
    sizes, refs, load, halo_send, x_send, up_send,
):
    (
        air_hbm, anbr_hbm, asend_hbm, amix_hbm, fw_hbm, counts_hbm, mw_hbm, owner_hbm,
        recv_hbm, sea_hbm, onbr_hbm, osend_hbm, omix_hbm, force_hbm, retw_hbm,
        air_out, sea_out, back_out, flux_out, force_out,
        anbr, asend, amix, fw, counts, mw, owner, recv, onbr, osend, omix, force, retw_in,
        pack, halo, gpack, ghalo, apool, gpool, opool, picker, amat, omat, member, ahead, early, lowmat, lowrow, spread, high,
        codes_out, codes_in, up_out, up_in, down_out, down_in, retw, slab, ret_bf, wide_force,
        halo_recv, x_recv, up_recv,
    ) = refs
    groups, devs, air_groups = sizes
    sea_groups = groups - air_groups
    g, d = lax.axis_index("grp"), lax.axis_index("dev")
    lower, upper = lax.rem(d + devs - 1, devs), lax.rem(d + 1, devs)
    is_air = g < air_groups
    mine = jnp.where(is_air, g, g - air_groups)
    half = halo.shape[2]
    capacity, block = recv.shape[2], recv.shape[4]
    span = capacity * block
    levels_a, columns = air_out.shape[2:]
    levels_o, cells = sea_out.shape[2:]
    fields = fw.shape[0]
    ret_fields = retw_in.shape[0]
    ret_pad = retw.shape[0]
    blocks = owner.shape[3]
    row_count = mw.shape[2]
    pairs = blocks // 2
    same = capacity == blocks
    base = lowmat.shape[0]
    bits = base.bit_length() - 1
    highs = cells // base
    field_pad = spread.shape[0] // highs
    width = high.shape[2]

    barrier = pltpu.get_barrier_semaphore()
    pl.semaphore_signal(barrier, inc=1, device_id={"dev": lower})
    pl.semaphore_signal(barrier, inc=1, device_id={"dev": upper})

    def loads(*copies):
        return [pltpu.make_async_copy(a, b, load.at[i]) for i, (a, b) in enumerate(copies)]

    def halos(source, target, levels, first):
        return [
            pltpu.make_async_remote_copy(
                src_ref=source.at[1 - side, :levels], dst_ref=target.at[side, :levels],
                send_sem=halo_send.at[first + side], recv_sem=halo_recv.at[first + side],
                device_id={"dev": upper if side == 0 else lower})
            for side in range(2)
        ]

    def code_copy(s, o):
        return pltpu.make_async_remote_copy(
            src_ref=codes_out, dst_ref=codes_in.at[s], send_sem=x_send.at[o],
            recv_sem=x_recv.at[s], device_id={"grp": air_groups + o})

    def down_copy(s, o):
        return pltpu.make_async_remote_copy(
            src_ref=down_out.at[s], dst_ref=down_in.at[o], send_sem=x_send.at[s],
            recv_sem=x_recv.at[o], device_id={"grp": s})

    def up_copy(s, p):
        return pltpu.make_async_remote_copy(
            src_ref=up_out.at[p], dst_ref=up_in.at[s, p], send_sem=up_send.at[0, p],
            recv_sem=up_recv.at[s, p], device_id={"grp": air_groups})

    def relay_copy(s, p):
        return pltpu.make_async_remote_copy(
            src_ref=up_in.at[s, p], dst_ref=up_in.at[s, p], send_sem=up_send.at[s, p],
            recv_sem=up_recv.at[s, p], device_id={"grp": g + 1})

    def packed(chosen, to, levels):
        to[0, :levels, :] = chosen[:, :half]
        to[1, :levels, :] = chosen[:, half:]

    def take_halo(copies, pool, levels, length, neighbours):
        for c in copies:
            c.wait()
        for side in range(2):
            at = slice(length + side * half, length + (side + 1) * half)
            pool[:, at] = scaled(halo[side, :levels, :], at.start, pool.shape[1], base_of(pool.shape[1]), neighbours)

    @pl.when(is_air)
    def _():
        for o in range(sea_groups):
            pl.semaphore_signal(barrier, inc=1, device_id={"grp": air_groups + o})
        (l_asend, l_air, l_fw, l_owner, l_counts, l_anbr, l_amix, l_mw, l_sea) = loads(
            (asend_hbm, asend), (air_hbm, air_out), (fw_hbm, fw), (owner_hbm, owner), (counts_hbm, counts),
            (anbr_hbm, anbr), (amix_hbm, amix), (mw_hbm, mw), (sea_hbm, sea_out))
        for c in (l_asend, l_fw, l_air, l_owner, l_counts, l_anbr, l_amix, l_mw):
            c.start()
        neighbours = anbr.shape[2]
        excess = row_count - columns
        tile = 256

        l_asend.wait()
        base_a = base_of(amat.shape[0])
        one_hot_matrix(picker.at[:columns], asend[0], base_of(columns))
        l_fw.wait()
        weight = two_parts(fw[...])
        l_air.wait()
        state = air_out[0, 0]
        top = state.astype(BF)
        own = joined(mm(weight, top) + mm(weight, (state - top.astype(F32)).astype(BF)))
        own_parts = two_parts(own)
        packed(mm(own_parts, picker[:columns]).astype(BF), gpack, 2 * fields)
        pl.semaphore_wait(barrier, 2 + sea_groups)
        near_sides = halos(gpack, ghalo, 2 * fields, 2)
        for c in near_sides:
            c.start()
        packed(mm(top, picker[:columns]).astype(BF), pack, levels_a)
        for h in range(columns // base_a):
            at = slice(h * base_a, (h + 1) * base_a)
            apool[:, at] = scaled(top[:, at], at.start, amat.shape[0], base_a, neighbours)
            gpool[:, at] = scaled(own_parts[:, at], at.start, amat.shape[0], base_a, neighbours)
        sides = halos(pack, halo, levels_a, 0)
        for c in sides:
            c.start()
        l_owner.wait()
        owners = [owner[0, 0, 0, b] for b in range(blocks)]
        slots = []
        for b in range(blocks):
            s = jnp.int32(b if same else 0)
            if not same:
                for e in range(b):
                    s = s + jnp.where(owners[e] == owners[b], 1, 0)
            slots.append(s)
        for b in range(blocks):
            codes_out[b : b + 1, :] = jnp.full((1, 128), owners[b] * capacity + slots[b], I32)
        if codes_out.shape[0] > blocks:
            codes_out[blocks:, :] = jnp.full((codes_out.shape[0] - blocks, 128), -1, I32)
        for o in range(sea_groups):
            code_copy(mine, o).start()
        l_sea.start()

        l_counts.wait()
        l_anbr.wait()
        l_amix.wait()
        l_mw.wait()
        column = row_columns(counts[...], row_count).astype(I32)
        low, high_of = column & (tile - 1), column >> (tile.bit_length() - 1)
        low_rows = as_rows(low, 16)

        def reach(p):
            first = max(0, p * tile - excess) // tile
            last = min(columns - 1, p * tile + tile - 1) // tile
            return range(first, last + 1)

        for p in range(row_count // tile):
            at = slice(p * tile, (p + 1) * tile)
            marks = [hot_rows(high_of[:, at], h, 16) for h in reach(p)]
            for t in range(tile // 16):
                part = low_hot(low_rows[:, at], t)
                for i, h in enumerate(reach(p)):
                    member[h * tile + t * 16 : h * tile + (t + 1) * 16, at] = part * marks[i]

        for c in range(columns // width):
            at = slice(c * width, (c + 1) * width)
            counts_matrix(amat, high, [anbr[0, 0, k : k + 1, at] for k in range(neighbours)], base_a, at)
        for c in range(columns // tile):
            at = slice(c * tile, (c + 1) * tile)
            mean = joined(mm(gpool[...], amat[:columns, at])) * (1.0 / neighbours)
            here, mix = own[:, at], amix[0, :, at]
            flux = here + mix * (mean - here)
            slab[: 2 * fields, at] = two_parts(flux)
            slab[2 * fields : 2 * fields + 16, at] = two_parts(jnp.broadcast_to(mix, (8, tile)))
        for p in range(row_count // tile):
            at = slice(p * tile, (p + 1) * tile)
            ks = reach(p)
            ks = slice(ks[0] * tile, (ks[-1] + 1) * tile)
            both = mm(slab[: 2 * fields + 16, ks], member[ks, at])
            share = mw[0, :, at]
            mix = joined(both[2 * fields :])[:1]
            early[:fields, at] = joined(both[: 2 * fields]) * share
            early[fields : fields + 8, at] = jnp.broadcast_to(share * mix * (1.0 / neighbours), (8, tile))
            ahead[:, at] = mm(amat[columns:, ks], member[ks, at]).astype(BF)
        for c in near_sides:
            c.wait()
        far = jnp.concatenate([
            scaled(ghalo[side], columns + side * half, amat.shape[0], base_a, neighbours) for side in range(2)], axis=1)
        for p in range(row_count // tile):
            at = slice(p * tile, (p + 1) * tile)
            values = early[:fields, at] + early[fields : fields + 1, at] * joined(mm(far, ahead[:, at]))
            per = tile // block
            for q in range(per // 2):
                b = slice(2 * q * block, (2 * q + 1) * block), slice((2 * q + 1) * block, (2 * q + 2) * block)
                up_out[p * (per // 2) + q] = jnp.concatenate([values[:, b[0]], values[:, b[1]]], axis=0).astype(BF)
                up_copy(mine, p * (per // 2) + q).start()
        take_halo(sides, apool, levels_a, columns, neighbours)
        for c in range(columns // width):
            at = slice(c * width, (c + 1) * width)
            mean = mm(apool[...], amat[:, at]) * (1.0 / neighbours)
            here = air_out[0, 0, :, at]
            air_out[0, 0, :, at] = here + amix[0, :, at] * (mean - here)
        for o in range(sea_groups):
            down_copy(0, o).wait_recv()
        for b in range(blocks):
            at = slice(b * block, (b + 1) * block)
            share = jnp.broadcast_to(mw[0, :, at], (ret_pad, block))
            value = down_in[owners[b], slots[b]].astype(F32) * share
            slab[: 2 * ret_pad, at] = two_parts(value)
            slab[2 * ret_pad : 4 * ret_pad, at] = two_parts(share)
        for c in range(columns // tile):
            at = slice(c * tile, (c + 1) * tile)
            rs = slice(c * tile, min(row_count, (c + 1) * tile + excess))
            sums = lax.dot_general(slab[: 4 * ret_pad, rs], member[at, rs], NT, preferred_element_type=F32)
            ratio = joined(sums[: 2 * ret_pad]) / joined(sums[2 * ret_pad :])
            for f in range(ret_fields):
                back_out[0, f, :, at] = ratio[f : f + 1]
        for o in range(sea_groups):
            code_copy(mine, o).wait_send()
        for p in range(pairs):
            up_copy(mine, p).wait_send()
        l_sea.wait()

    @pl.when(jnp.logical_not(is_air))
    def _():
        for s in range(air_groups):
            pl.semaphore_signal(barrier, inc=1, device_id={"grp": s})
        not_first, not_last = mine > 0, mine < sea_groups - 1

        @pl.when(not_first)
        def _():
            pl.semaphore_signal(barrier, inc=1, device_id={"grp": g - 1})

        @pl.when(not_last)
        def _():
            pl.semaphore_signal(barrier, inc=1, device_id={"grp": g + 1})

        (l_osend, l_sea, l_retw, l_recv, l_onbr, l_omix, l_force, l_air) = loads(
            (osend_hbm, osend), (sea_hbm, sea_out), (retw_hbm, retw_in), (recv_hbm, recv), (onbr_hbm, onbr),
            (omix_hbm, omix), (force_hbm, force), (air_hbm, air_out))
        for c in (l_osend, l_sea, l_retw, l_recv, l_onbr, l_omix, l_force):
            c.start()
        neighbours = onbr.shape[1]
        l_osend.wait()
        one_hot_matrix(picker.at[:cells], osend[0], base)
        base_p = base_of(omat.shape[0])
        l_sea.wait()
        top = sea_out[0, 0].astype(BF)
        packed(mm(top, picker[:cells]).astype(BF), pack, levels_o)
        links = jnp.where(not_first, 1, 0) + jnp.where(not_last, 1, 0)
        pl.semaphore_wait(barrier, 2 + air_groups + links)
        sides = halos(pack, halo, levels_o, 0)
        for c in sides:
            c.start()
        l_air.start()
        l_retw.wait()
        l_recv.wait()
        l_onbr.wait()
        l_omix.wait()
        l_force.wait()
        retw[...] = jnp.zeros(retw.shape, F32)
        retw[:ret_fields] = retw_in[...]
        weight = two_parts(retw[...])
        state = sea_out[0, 0]
        top = state.astype(BF)
        rest = (state - top.astype(F32)).astype(BF)
        for h in range(cells // base_p):
            at = slice(h * base_p, (h + 1) * base_p)
            opool[:, at] = scaled(top[:, at], at.start, omat.shape[0], base_p, neighbours)
        returned = joined(mm(weight, top) + mm(weight, rest)).astype(BF)
        for h in range(highs):
            ret_bf[h * ret_pad : (h + 1) * ret_pad] = returned[:, h * base : (h + 1) * base]

        def slot_ids(s):
            return jnp.concatenate([recv[0, 0, k, s : s + 1, :] for k in range(capacity)], axis=1)

        for s in range(air_groups):
            idx = slot_ids(s)
            at = slice(s * span, (s + 1) * span)
            low = as_rows(idx & (base - 1), 16)
            for t in range(base // 16):
                lowmat[t * 16 : (t + 1) * 16, at] = low_hot(low, t)
            found = mm(ret_bf[...], lowmat[:, at])
            high_of = jnp.broadcast_to(idx >> bits, (ret_pad, span))
            looked = jnp.zeros((ret_pad, span), F32)
            for h in range(highs):
                looked = jnp.where(high_of == h, found[h * ret_pad : (h + 1) * ret_pad], looked)
            for k in range(capacity):
                down_out[s, k] = looked[:, k * block : (k + 1) * block].astype(BF)
            down_copy(s, mine).start()
        wide_force[...] = jnp.zeros(wide_force.shape, F32)
        strong = force[...]
        wide_force[:fields, :levels_o] = strong
        wide_force[field_pad : field_pad + fields, :levels_o] = strong
        wide_force[2 * field_pad : 2 * field_pad + fields, :levels_o] = strong - strong.astype(BF).astype(F32)
        force_out[...] = wide_force[...].T.astype(BF)
        flux_out[...] = jnp.zeros(flux_out.shape, F32)
        back_out[...] = jnp.zeros(back_out.shape, F32)
        tiles = cells // width
        row_span = blocks * block
        near = lowmat if same else lowrow

        def build(c):
            at = slice(c * width, (c + 1) * width)
            counts_matrix(omat, high, [onbr[0, k, :, at] for k in range(neighbours)], base_p, at)

        def product(c, depth):
            at = slice(c * width, (c + 1) * width)
            mean = mm(opool[:, :depth], omat[:depth, at]) * (1.0 / neighbours)
            here = sea_out[0, 0, :, at]
            sea_out[0, 0, :, at] = here + omix[0, :, at] * (mean - here)

        def rim(c):
            at = slice(c * width, (c + 1) * width)
            mean = mm(opool[:, cells:], omat[cells:, at]) * (1.0 / neighbours)
            sea_out[0, 0, :, at] += omix[0, :, at] * mean

        def relay(p):
            for s in range(air_groups):
                relay_copy(s, p).wait_recv()

                @pl.when(not_last)
                def _():
                    relay_copy(s, p).start()

        rows_high = []

        def code():
            for s in range(air_groups):
                code_copy(s, 0).wait_recv()
                place = codes_in[s] - mine * capacity
                ids = []
                for b in range(blocks):
                    here = place[b : b + 1]
                    held = (here >= 0) & (here < capacity)
                    if same:
                        cell = recv[0, 0, b, s : s + 1, :]
                    else:
                        cell = jnp.zeros((1, block), I32)
                        for k in range(capacity):
                            cell = jnp.where(here == k, recv[0, 0, k, s : s + 1, :], cell)
                    ids.append(jnp.where(held, cell, -1))
                rows_high.append([i >> bits for i in ids])
                if not same:
                    low = as_rows(jnp.concatenate(ids, axis=1) & (base - 1), 16)
                    for t in range(base // 16):
                        lowrow[t * 16 : (t + 1) * 16, s * row_span : (s + 1) * row_span] = low_hot(low, t)

        def collect(p):
            total = flux_out[...]
            for s in range(air_groups):
                arrived = up_in[s, p].astype(F32)
                for j in range(2):
                    at = slice(s * row_span + (2 * p + j) * block, s * row_span + (2 * p + j + 1) * block)
                    part = jnp.concatenate(
                        [arrived[j * fields : (j + 1) * fields], jnp.zeros((field_pad - fields, block), F32)], axis=0)
                    high_of = jnp.broadcast_to(rows_high[s][2 * p + j], (field_pad, block))
                    for h in range(highs):
                        spread[h * field_pad : (h + 1) * field_pad, at] = (
                            jnp.where(high_of == h, part, 0.0).astype(BF))
                at = slice(s * row_span + 2 * p * block, s * row_span + (2 * p + 2) * block)
                total = total + lax.dot_general(spread[:, at], near[:, at], NT, preferred_element_type=F32)
            flux_out[...] = total

        build(0)
        late = min(5, tiles)
        for c in range(late):
            product(c, cells)
            if c + 1 < tiles:
                build(c + 1)
        take_halo(sides, opool, levels_o, cells, neighbours)
        for c in range(late):
            rim(c)
        for c in range(late, tiles):
            product(c, omat.shape[0])
            if c + 1 < tiles:
                build(c + 1)
        code()
        relay(0)
        for p in range(pairs):
            if p:
                relay(p)
            collect(p)
        for s in range(air_groups):
            down_copy(s, mine).wait_send()

        @pl.when(not_last)
        def _():
            for p in range(pairs):
                for s in range(air_groups):
                    relay_copy(s, p).wait_send()

        l_air.wait()


def finish(air_groups, a, b, c, flux, force, a_out, b_out, c_out, held, sem):
    is_air = lax.axis_index("grp") < air_groups
    base, field_pad = flux.shape[1], force.shape[1] // 4
    highs = flux.shape[0] // field_pad
    levels = b.shape[2]
    first = pltpu.make_async_copy(a, a_out, sem.at[0])
    last = pltpu.make_async_copy(c, c_out, sem.at[1])
    first.start()
    last.start()

    @pl.when(is_air)
    def _():
        whole = pltpu.make_async_copy(b, b_out, sem.at[2])
        whole.start()
        whole.wait()

    @pl.when(jnp.logical_not(is_air))
    def _():
        copies = []
        steps = 4 if highs % 4 == 0 else 1
        for i in range(steps):
            for h in range(i * highs // steps, (i + 1) * highs // steps):
                at = slice(h * base, (h + 1) * base)
                here = flux[h * field_pad : (h + 1) * field_pad]
                top = here.astype(BF)
                rest = (here - top.astype(F32)).astype(BF)
                three = jnp.concatenate([top, rest, top], axis=0)
                held[0, 0, :, at] = b[0, 0, :, at] + mm(force[:levels, : 3 * field_pad], three)
            at = slice(i * highs // steps * base, (i + 1) * highs // steps * base)
            copies.append(pltpu.make_async_copy(held.at[0, 0, :, at], b_out.at[0, 0, :, at], sem.at[2 + i]))
            copies[-1].start()
        for x in copies:
            x.wait()

    first.wait()
    last.wait()


def solution(mesh):
    groups, devs = mesh.shape["grp"], mesh.shape["dev"]
    in_specs = (
        P("grp", "dev", None, None), P("grp", "dev", None, None), P("grp", "dev", None),
        P("grp", "dev", None), P(), P("grp", "dev", None), P("grp", "dev", None),
        P("grp", "dev", None, None), P("grp", "dev", None, None, None),
        P("grp", "dev", None, None), P("grp", "dev", None, None), P("grp", "dev", None),
        P("grp", "dev", None), P(), P(),
    )
    out_specs = (P("grp", "dev", None, None),) * 3

    def on_device(*args):
        args = list(args)
        args[5] = args[5].reshape(-1, 128)
        args[7] = args[7].transpose(0, 1, 3, 2)
        args[8] = args[8].transpose(0, 1, 3, 2, 4)
        args[10] = args[10].transpose(0, 2, 1, 3)
        args[13] = args[13].T
        air, anbr, asend, amix, fw, counts, mw, owner, recv, sea, onbr, osend, omix, force, ret = args
        levels_a, columns = air.shape[2:]
        levels_o, cells = sea.shape[2:]
        half = asend.shape[2] // 2
        capacity, air_groups, block = recv.shape[2:]
        sea_groups = groups - air_groups
        blocks = owner.shape[3]
        fields, ret_fields = fw.shape[0], ret.shape[0]
        ret_pad = -(-ret_fields // 16) * 16
        field_pad = -(-fields // 16) * 16
        row_count = mw.shape[2]
        pairs = blocks // 2
        pool_a, pool_o = columns + 2 * half, cells + 2 * half
        width = 256
        base, span = base_of(cells), air_groups * capacity * block
        row_span = air_groups * blocks * block
        same = capacity == blocks
        deep = max(
            anbr.shape[2] * (pool_a // base_of(pool_a)),
            onbr.shape[1] * (pool_o // base_of(pool_o)),
        )
        code_rows = -(-blocks // 8) * 8
        V = pltpu.VMEM
        dma = pltpu.SemaphoreType.DMA
        kept = [V(x.shape, x.dtype) for x in (anbr, asend, amix, fw, counts, mw)]
        kept += [pltpu.SMEM(owner.shape, owner.dtype)]
        kept += [V(x.shape, x.dtype) for x in (recv, onbr, osend, omix, force, ret)]
        levels = max(levels_a, levels_o)
        scratch = kept + [
            V((2, levels, half), BF), V((2, levels, half), BF),
            V((2, 2 * fields, half), BF), V((2, 2 * fields, half), BF),
            V((levels_a, pool_a), BF), V((2 * fields, columns), BF), V((levels_o, pool_o), BF), V((max(columns, cells), 2 * half), BF),
            V((pool_a, columns), BF), V((pool_o, cells), BF),
            V((columns, row_count), BF), V((2 * half, row_count), BF), V((fields + 8, row_count), F32),
            V((base, span), BF),
            V((base if not same else 16, row_span if not same else 128), BF),
            V((cells // base * field_pad, row_span), BF),
            V((deep, 16, width), BF),
            V((code_rows, 128), I32), V((air_groups, code_rows, 128), I32),
            V((pairs, 2 * fields, block), BF), V((air_groups, pairs, 2 * fields, block), BF),
            V((air_groups, capacity, ret_pad, block), BF), V((sea_groups, capacity, ret_pad, block), BF),
            V((ret_pad, levels_o), F32),
            V((max(4 * ret_pad, 2 * fields + 16), max(row_count, columns)), BF),
            V((cells // base * ret_pad, base), BF),
            V((4 * field_pad, 128), F32),
            dma((4,)), dma((max(air_groups, sea_groups),)), dma((air_groups, pairs)),
        ]
        sends = ((9,), (4,), (max(air_groups, sea_groups),), (air_groups, pairs))
        vmem = pl.BlockSpec(memory_space=pltpu.VMEM)
        outs = (
            jax.ShapeDtypeStruct(air.shape, F32),
            jax.ShapeDtypeStruct(sea.shape, F32),
            jax.ShapeDtypeStruct((1, ret_fields, 1, columns), F32),
        )
        kept_outs = outs + (
            jax.ShapeDtypeStruct((cells // base * field_pad, base), F32),
            jax.ShapeDtypeStruct((128, 4 * field_pad), BF),
        )
        parts = pl.pallas_call(
            functools.partial(kernel, (groups, devs, air_groups, sends)),
            out_shape=kept_outs,
            in_specs=[pl.BlockSpec(memory_space=pltpu.HBM)] * 15,
            out_specs=(vmem,) * 5,
            scratch_shapes=scratch,
            compiler_params=pltpu.CompilerParams(
                collective_id=0, has_side_effects=True, vmem_limit_bytes=48 * 1024 * 1024),
            name="couple",
        )(*[pltpu.with_memory_space_constraint(x, pltpu.HBM) for x in args])
        air_next, sea_next, back = pl.pallas_call(
            functools.partial(finish, air_groups),
            out_shape=outs,
            in_specs=[vmem] * 5,
            out_specs=(pl.BlockSpec(memory_space=pl.ANY),) * 3,
            scratch_shapes=[V(sea.shape, F32), dma((6,))],
            compiler_params=pltpu.CompilerParams(vmem_limit_bytes=4 * 1024 * 1024),
            name="finish",
        )(*parts)
        return air_next, sea_next, back.transpose(0, 2, 1, 3)

    return jax.shard_map(
        on_device, mesh=mesh, in_specs=in_specs, out_specs=out_specs, check_vma=False)
```

```python
import functools

import jax
import jax.numpy as jnp
from jax import lax
from jax.experimental import pallas as pl
from jax.experimental.pallas import tpu as pltpu
from jax.sharding import PartitionSpec as P

EXACT = lax.Precision.HIGHEST
BF = jnp.bfloat16
F32 = jnp.float32
I32 = jnp.int32
NT = (((1,), (1,)), ((), ()))
TN = (((0,), (0,)), ((), ()))


def mm(a, b):
    return jnp.dot(a, b, preferred_element_type=F32)


def two_parts(x):
    rest = x - x.astype(BF).astype(F32)
    return jnp.concatenate([x, rest], axis=0).astype(BF)


def joined(x):
    half = x.shape[0] // 2
    return x[:half] + x[half:]


def low_hot(low, t):
    place = lax.broadcasted_iota(I32, low.shape, 0).astype(F32) + 16.0 * t
    return jnp.where(low == place.astype(BF), jnp.asarray(1, BF), jnp.asarray(0, BF))


def as_rows(idx, rows):
    return jnp.broadcast_to(idx.astype(F32), (rows, idx.shape[1])).astype(BF)


def hot_rows(high, h, rows):
    return jnp.where(as_rows(high, rows) == jnp.asarray(h, BF), jnp.asarray(1, BF), jnp.asarray(0, BF))


def one_hot_matrix(out_ref, idx, base):
    bits = base.bit_length() - 1
    low = as_rows(idx & (base - 1), 16)
    marks = [hot_rows(idx >> bits, h, 16) for h in range(out_ref.shape[0] // base)]
    for t in range(base // 16):
        part = low_hot(low, t)
        for h, mark in enumerate(marks):
            out_ref[h * base + t * 16 : h * base + (t + 1) * 16, :] = part * mark


def couples(highs, neighbours):
    step = 2 if neighbours < 8 else 1
    return [tuple(range(h, min(h + step, highs))) for h in range(0, highs, step)]


def scale_at(position, length, base, neighbours):
    for couple in couples(length // base, neighbours):
        if position // base in couple:
            return 16.0 if len(couple) == 2 and position // base == couple[0] else 1.0


def scaled(x, at, length, base, neighbours):
    return x * jnp.asarray(scale_at(at, length, base, neighbours), BF)


def counts_matrix(out_ref, high_ref, idx_rows, base, at):
    highs = out_ref.shape[0] // base
    bits = base.bit_length() - 1
    lines = couples(highs, len(idx_rows))
    low = [as_rows(i & (base - 1), 16) for i in idx_rows]
    for k, i in enumerate(idx_rows):
        top = as_rows(i >> bits, 16)
        for n, couple in enumerate(lines):
            mark = jnp.where(top == jnp.asarray(couple[-1], BF), jnp.asarray(1, BF), jnp.asarray(0, BF))
            if len(couple) == 2:
                mark = jnp.where(top == jnp.asarray(couple[0], BF), jnp.asarray(1 / 16, BF), mark)
            high_ref[k * len(lines) + n] = mark
    for t in range(base // 16):
        parts = [low_hot(i, t) for i in low]
        for n, couple in enumerate(lines):
            total = parts[0] * high_ref[n]
            for k in range(1, len(parts)):
                total = total + parts[k] * high_ref[k * len(lines) + n]
            if len(couple) == 2:
                whole = (total + jnp.asarray(128, BF)) - jnp.asarray(128, BF)
                out_ref[couple[0] * base + t * 16 : couple[0] * base + (t + 1) * 16, at] = total - whole
                total = whole
            out_ref[couple[-1] * base + t * 16 : couple[-1] * base + (t + 1) * 16, at] = total


def base_of(length):
    return 256 if length % 256 == 0 else 128


def row_columns(counts, rows):
    lines = counts.shape[0]
    wide = jnp.concatenate([counts.astype(F32), jnp.zeros((-lines % 16, 128), F32)], axis=0).astype(BF)
    lines = wide.shape[0]
    i = lax.broadcasted_iota(I32, (128, 128), 0)
    j = lax.broadcasted_iota(I32, (128, 128), 1)
    within = mm(wide, jnp.where(i <= j, 1.0, 0.0).astype(BF))
    i = lax.broadcasted_iota(I32, (lines, lines), 0)
    j = lax.broadcasted_iota(I32, (lines, lines), 1)
    ones = jnp.ones((128, 128), BF)
    before = mm(mm(jnp.where(j < i, 1.0, 0.0).astype(BF), wide).astype(BF), ones)
    upto = mm(mm(jnp.where(j <= i, 1.0, 0.0).astype(BF), wide).astype(BF), ones)
    offsets = within + before
    high = jnp.floor(offsets * (1.0 / 256.0)) * 256.0
    halves = jnp.concatenate([high, offsets - high], axis=0).astype(BF)
    tiles = rows // 128
    at = lax.broadcasted_iota(I32, (lines, rows), 1).astype(F32)
    ends = jnp.concatenate([upto] * tiles, axis=1)
    starts = jnp.concatenate([before] * tiles, axis=1)
    passed = jnp.where(ends <= at, 1.0, 0.0)
    line = jnp.where(starts <= at, 1.0, 0.0) - passed
    line = jnp.concatenate([line, line], axis=0).astype(BF)
    ends_in = lax.dot_general(halves, line, TN, preferred_element_type=F32)
    at = lax.broadcasted_iota(I32, (128, rows), 1).astype(F32)
    inner = jnp.sum(jnp.where(ends_in <= at, 1.0, 0.0), axis=0, keepdims=True)
    return 128.0 * jnp.sum(passed, axis=0, keepdims=True) + inner


def kernel(sizes, *refs):
    pl.run_scoped(
        functools.partial(body, sizes[:3], refs),
        *(pltpu.SemaphoreType.DMA(n) for n in sizes[3]))


def body(
    sizes, refs, load, halo_send, x_send, up_send,
):
    (
        air_hbm, anbr_hbm, asend_hbm, amix_hbm, fw_hbm, counts_hbm, mw_hbm, owner_hbm,
        recv_hbm, sea_hbm, onbr_hbm, osend_hbm, omix_hbm, force_hbm, retw_hbm,
        air_out, sea_out, back_out, flux_out, force_out,
        anbr, asend, amix, fw, counts, mw, owner, recv, onbr, osend, omix, force, retw_in,
        pack, halo, gpack, ghalo, apool, gpool, opool, picker, amat, omat, member, ahead, early, lowmat, lowrow, spread, high,
        codes_out, codes_in, up_out, up_in, down_out, down_in, retw, slab, ret_bf, wide_force,
        halo_recv, x_recv, up_recv, told,
    ) = refs
    groups, devs, air_groups = sizes
    sea_groups = groups - air_groups
    g, d = lax.axis_index("grp"), lax.axis_index("dev")
    lower, upper = lax.rem(d + devs - 1, devs), lax.rem(d + 1, devs)
    is_air = g < air_groups
    mine = jnp.where(is_air, g, g - air_groups)
    half = halo.shape[2]
    capacity, block = recv.shape[2], recv.shape[4]
    span = capacity * block
    levels_a, columns = air_out.shape[2:]
    levels_o, cells = sea_out.shape[2:]
    fields = fw.shape[0]
    ret_fields = retw_in.shape[0]
    ret_pad = retw.shape[0]
    blocks = owner.shape[3]
    row_count = mw.shape[2]
    pairs = blocks // 2
    same = capacity == blocks
    base = lowmat.shape[0]
    bits = base.bit_length() - 1
    highs = cells // base
    field_pad = spread.shape[0] // highs
    width = high.shape[2]

    barrier = pltpu.get_barrier_semaphore()
    pl.semaphore_signal(barrier, inc=1, device_id={"dev": lower})
    pl.semaphore_signal(barrier, inc=1, device_id={"dev": upper})

    def loads(*copies):
        return [pltpu.make_async_copy(a, b, load.at[i]) for i, (a, b) in enumerate(copies)]

    def halos(source, target, levels, first):
        return [
            pltpu.make_async_remote_copy(
                src_ref=source.at[1 - side, :levels], dst_ref=target.at[side, :levels],
                send_sem=halo_send.at[first + side], recv_sem=halo_recv.at[first + side],
                device_id={"dev": upper if side == 0 else lower})
            for side in range(2)
        ]

    def code_copy(s):
        return pltpu.make_async_remote_copy(
            src_ref=codes_out, dst_ref=codes_in.at[s], send_sem=x_send.at[0],
            recv_sem=x_recv.at[s], device_id={"grp": air_groups})

    def code_relay(s):
        return pltpu.make_async_remote_copy(
            src_ref=codes_in.at[s], dst_ref=codes_in.at[s], send_sem=x_send.at[air_groups + s],
            recv_sem=x_recv.at[s], device_id={"grp": g + 1})

    def down_copy(s, o):
        return pltpu.make_async_remote_copy(
            src_ref=down_out.at[s], dst_ref=down_in.at[o], send_sem=x_send.at[s],
            recv_sem=x_recv.at[o], device_id={"grp": s})

    def up_copy(s, p):
        return pltpu.make_async_remote_copy(
            src_ref=up_out.at[p], dst_ref=up_in.at[s, p], send_sem=up_send.at[0, p],
            recv_sem=up_recv.at[s, p], device_id={"grp": air_groups})

    def relay_copy(s, p):
        return pltpu.make_async_remote_copy(
            src_ref=up_in.at[s, p], dst_ref=up_in.at[s, p], send_sem=up_send.at[s, p],
            recv_sem=up_recv.at[s, p], device_id={"grp": g + 1})

    def packed(chosen, to, levels):
        to[0, :levels, :] = chosen[:, :half]
        to[1, :levels, :] = chosen[:, half:]

    def take_halo(copies, pool, levels, length, neighbours):
        for c in copies:
            c.wait()
        for side in range(2):
            at = slice(length + side * half, length + (side + 1) * half)
            pool[:, at] = scaled(halo[side, :levels, :], at.start, pool.shape[1], base_of(pool.shape[1]), neighbours)

    @pl.when(is_air)
    def _():
        pl.semaphore_signal(barrier, inc=1, device_id={"grp": air_groups})
        (l_asend, l_air, l_fw, l_owner, l_counts, l_anbr, l_amix, l_mw, l_sea) = loads(
            (asend_hbm, asend), (air_hbm, air_out), (fw_hbm, fw), (owner_hbm, owner), (counts_hbm, counts),
            (anbr_hbm, anbr), (amix_hbm, amix), (mw_hbm, mw), (sea_hbm, sea_out))
        for c in (l_asend, l_air, l_fw, l_anbr, l_counts, l_amix, l_mw, l_owner):
            c.start()
        neighbours = anbr.shape[2]
        excess = row_count - columns
        tile = 256

        l_asend.wait()
        base_a = base_of(amat.shape[0])
        one_hot_matrix(picker.at[:columns], asend[0], base_of(columns))
        l_fw.wait()
        weight = two_parts(fw[...])
        l_air.wait()
        state = air_out[0, 0]
        top = state.astype(BF)
        own = joined(mm(weight, top) + mm(weight, (state - top.astype(F32)).astype(BF)))
        own_parts = two_parts(own)
        packed(mm(own_parts, picker[:columns]).astype(BF), gpack, 2 * fields)
        pl.semaphore_wait(barrier, 3)
        near_sides = halos(gpack, ghalo, 2 * fields, 2)
        for c in near_sides:
            c.start()
        l_owner.wait()
        owners = [owner[0, 0, 0, b] for b in range(blocks)]
        slots = []
        for b in range(blocks):
            s = jnp.int32(b if same else 0)
            if not same:
                for e in range(b):
                    s = s + jnp.where(owners[e] == owners[b], 1, 0)
            slots.append(s)
        for b in range(blocks):
            codes_out[b : b + 1, :] = jnp.full((1, 128), owners[b] * capacity + slots[b], I32)
        if codes_out.shape[0] > blocks:
            codes_out[blocks:, :] = jnp.full((codes_out.shape[0] - blocks, 128), -1, I32)
        code_copy(mine).start()
        l_sea.start()

        l_anbr.wait()
        l_amix.wait()
        l_mw.wait()
        for c in range(columns // width):
            at = slice(c * width, (c + 1) * width)
            counts_matrix(amat, high, [anbr[0, 0, k : k + 1, at] for k in range(neighbours)], base_a, at)
        for h in range(columns // base_a):
            at = slice(h * base_a, (h + 1) * base_a)
            apool[:, at] = scaled(top[:, at], at.start, amat.shape[0], base_a, neighbours)
            gpool[:, at] = scaled(own_parts[:, at], at.start, amat.shape[0], base_a, neighbours)
        for c in range(columns // tile):
            at = slice(c * tile, (c + 1) * tile)
            mean = joined(mm(gpool[...], amat[:columns, at])) * (1.0 / neighbours)
            here, mix = own[:, at], amix[0, :, at]
            flux = here + mix * (mean - here)
            slab[: 2 * fields, at] = two_parts(flux)
            slab[2 * fields : 2 * fields + 16, at] = two_parts(jnp.broadcast_to(mix, (8, tile)))
        l_counts.wait()
        column = row_columns(counts[...], row_count).astype(I32)
        low, high_of = column & (tile - 1), column >> (tile.bit_length() - 1)
        low_rows = as_rows(low, 16)

        def reach(p):
            first = max(0, p * tile - excess) // tile
            last = min(columns - 1, p * tile + tile - 1) // tile
            return range(first, last + 1)

        for p in range(row_count // tile):
            at = slice(p * tile, (p + 1) * tile)
            marks = [hot_rows(high_of[:, at], h, 16) for h in reach(p)]
            for t in range(tile // 16):
                part = low_hot(low_rows[:, at], t)
                for i, h in enumerate(reach(p)):
                    member[h * tile + t * 16 : h * tile + (t + 1) * 16, at] = part * marks[i]

        for p in range(row_count // tile):
            at = slice(p * tile, (p + 1) * tile)
            ks = reach(p)
            ks = slice(ks[0] * tile, (ks[-1] + 1) * tile)
            both = mm(jnp.concatenate([slab[: 2 * fields + 16, ks], amat[columns:, ks]], axis=0), member[ks, at])
            share = mw[0, :, at]
            mix = joined(both[2 * fields : 2 * fields + 16])[:1]
            early[:fields, at] = joined(both[: 2 * fields]) * share
            early[fields : fields + 8, at] = jnp.broadcast_to(share * mix * (1.0 / neighbours), (8, tile))
            ahead[:, at] = both[2 * fields + 16 :].astype(BF)
        for c in near_sides:
            c.wait()
        far = jnp.concatenate([
            scaled(ghalo[side], columns + side * half, amat.shape[0], base_a, neighbours) for side in range(2)], axis=1)
        for p in range(row_count // tile):
            at = slice(p * tile, (p + 1) * tile)
            values = early[:fields, at] + early[fields : fields + 1, at] * joined(mm(far, ahead[:, at]))
            per = tile // block
            for q in range(per // 2):
                b = slice(2 * q * block, (2 * q + 1) * block), slice((2 * q + 1) * block, (2 * q + 2) * block)
                whole = fields - fields % 16
                up_out[p * (per // 2) + q] = jnp.concatenate(
                    [values[f, at] for f in (slice(whole), slice(whole, None)) for at in b], axis=0).astype(BF)
                up_copy(mine, p * (per // 2) + q).start()
        packed(mm(air_out[0, 0].astype(BF), picker[:columns]).astype(BF), pack, levels_a)
        sides = halos(pack, halo, levels_a, 0)
        for c in sides:
            c.start()
        take_halo(sides, apool, levels_a, columns, neighbours)
        for c in range(columns // width):
            at = slice(c * width, (c + 1) * width)
            mean = mm(apool[...], amat[:, at]) * (1.0 / neighbours)
            here = air_out[0, 0, :, at]
            air_out[0, 0, :, at] = here + amix[0, :, at] * (mean - here)
        for o in range(sea_groups):
            down_copy(0, o).wait_recv()
        for b in range(blocks):
            at = slice(b * block, (b + 1) * block)
            share = jnp.broadcast_to(mw[0, :, at], (ret_pad, block))
            value = down_in[owners[b], slots[b]].astype(F32) * share
            slab[: 2 * ret_pad, at] = two_parts(value)
            slab[2 * ret_pad : 4 * ret_pad, at] = two_parts(share)
        for c in range(columns // tile):
            at = slice(c * tile, (c + 1) * tile)
            rs = slice(c * tile, min(row_count, (c + 1) * tile + excess))
            sums = lax.dot_general(slab[: 4 * ret_pad, rs], member[at, rs], NT, preferred_element_type=F32)
            ratio = joined(sums[: 2 * ret_pad]) / joined(sums[2 * ret_pad :])
            for f in range(ret_fields):
                back_out[0, f, :, at] = ratio[f : f + 1]
        code_copy(mine).wait_send()
        for p in range(pairs):
            up_copy(mine, p).wait_send()
        l_sea.wait()

    @pl.when(jnp.logical_not(is_air))
    def _():
        not_first, not_last = mine > 0, mine < sea_groups - 1

        @pl.when(not_first)
        def _():
            pl.semaphore_signal(barrier, inc=1, device_id={"grp": g - 1})

        @pl.when(jnp.logical_not(not_first))
        def _():
            for s in range(air_groups):
                pl.semaphore_signal(barrier, inc=1, device_id={"grp": s})

        @pl.when(not_last)
        def _():
            pl.semaphore_signal(barrier, inc=1, device_id={"grp": g + 1})

        (l_osend, l_sea, l_retw, l_recv, l_onbr, l_omix, l_force, l_air) = loads(
            (osend_hbm, osend), (sea_hbm, sea_out), (retw_hbm, retw_in), (recv_hbm, recv), (onbr_hbm, onbr),
            (omix_hbm, omix), (force_hbm, force), (air_hbm, air_out))
        for c in (l_osend, l_sea, l_retw, l_recv, l_onbr, l_omix, l_force):
            c.start()
        neighbours = onbr.shape[1]
        l_osend.wait()
        one_hot_matrix(picker.at[:cells], osend[0], base)
        base_p = base_of(omat.shape[0])
        l_sea.wait()
        top = sea_out[0, 0].astype(BF)
        packed(mm(top, picker[:cells]).astype(BF), pack, levels_o)
        links = jnp.where(not_first, 1, air_groups) + jnp.where(not_last, 1, 0)
        pl.semaphore_wait(barrier, 2 + links)
        sides = halos(pack, halo, levels_o, 0)
        for c in sides:
            c.start()

        @pl.when(not_first)
        def _():
            pl.semaphore_wait(told, 1)

        @pl.when(not_last)
        def _():
            pl.semaphore_signal(told, inc=1, device_id={"grp": g + 1})

        l_air.start()
        l_retw.wait()
        l_recv.wait()
        l_onbr.wait()
        l_omix.wait()
        l_force.wait()
        retw[...] = jnp.zeros(retw.shape, F32)
        retw[:ret_fields] = retw_in[...]
        weight = two_parts(retw[...])
        state = sea_out[0, 0]
        top = state.astype(BF)
        rest = (state - top.astype(F32)).astype(BF)
        for h in range(cells // base_p):
            at = slice(h * base_p, (h + 1) * base_p)
            opool[:, at] = scaled(top[:, at], at.start, omat.shape[0], base_p, neighbours)
        returned = joined(mm(weight, top) + mm(weight, rest)).astype(BF)
        for h in range(highs):
            ret_bf[h * ret_pad : (h + 1) * ret_pad] = returned[:, h * base : (h + 1) * base]

        def slot_ids(s):
            return jnp.concatenate([recv[0, 0, k, s : s + 1, :] for k in range(capacity)], axis=1)

        for s in range(air_groups):
            idx = slot_ids(s)
            at = slice(s * span, (s + 1) * span)
            low = as_rows(idx & (base - 1), 16)
            for t in range(base // 16):
                lowmat[t * 16 : (t + 1) * 16, at] = low_hot(low, t)
            found = mm(ret_bf[...], lowmat[:, at])
            high_of = jnp.broadcast_to(idx >> bits, (ret_pad, span))
            looked = jnp.zeros((ret_pad, span), F32)
            for h in range(highs):
                looked = jnp.where(high_of == h, found[h * ret_pad : (h + 1) * ret_pad], looked)
            for k in range(capacity):
                down_out[s, k] = looked[:, k * block : (k + 1) * block].astype(BF)
            down_copy(s, mine).start()
        wide_force[...] = jnp.zeros(wide_force.shape, F32)
        strong = force[...]
        for i, part in enumerate((strong, strong, strong - strong.astype(BF).astype(F32))):
            wide_force[i * field_pad : i * field_pad + fields, :levels_o] = part
            wide_force[i * field_pad + fields : (i + 1) * field_pad, :levels_o] = part[fields - fields % 16 :]
        force_out[...] = wide_force[...].T.astype(BF)
        flux_out[...] = jnp.zeros(flux_out.shape, F32)
        back_out[...] = jnp.zeros(back_out.shape, F32)
        tiles = cells // width
        row_span = blocks * block
        near = lowmat if same else lowrow

        def build(c):
            at = slice(c * width, (c + 1) * width)
            counts_matrix(omat, high, [onbr[0, k, :, at] for k in range(neighbours)], base_p, at)

        def product(c, depth):
            at = slice(c * width, (c + 1) * width)
            mean = mm(opool[:, :depth], omat[:depth, at]) * (1.0 / neighbours)
            here = sea_out[0, 0, :, at]
            sea_out[0, 0, :, at] = here + omix[0, :, at] * (mean - here)

        def rim(c):
            at = slice(c * width, (c + 1) * width)
            mean = mm(opool[:, cells:], omat[cells:, at]) * (1.0 / neighbours)
            sea_out[0, 0, :, at] += omix[0, :, at] * mean

        rows_high = []
        whole = fields - fields % 16
        zero = jnp.asarray(0, BF)
        lines = lax.broadcasted_iota(I32, (16, block), 0)
        side = [jnp.where((lines >= 8 * j) & (lines < 8 * j + 8), 1.0, 0.0).astype(BF) for j in range(2)]

        def code():
            @pl.when(jnp.logical_not(not_last))
            def _():
                for s in range(air_groups):
                    code_relay(s).wait_recv()

            for s in range(air_groups):
                place = codes_in[s] - mine * capacity
                ids = []
                for b in range(blocks):
                    here = place[b : b + 1]
                    held = (here >= 0) & (here < capacity)
                    if same:
                        cell = recv[0, 0, b, s : s + 1, :]
                    else:
                        cell = jnp.zeros((1, block), I32)
                        for k in range(capacity):
                            cell = jnp.where(here == k, recv[0, 0, k, s : s + 1, :], cell)
                    ids.append(jnp.where(held, cell, -1))
                rows_high.append([as_rows(i >> bits, 16) for i in ids])
                if not same:
                    low = as_rows(jnp.concatenate(ids, axis=1) & (base - 1), 16)
                    for t in range(base // 16):
                        lowrow[t * 16 : (t + 1) * 16, s * row_span : (s + 1) * row_span] = low_hot(low, t)

        def collect(some):
            total = flux_out[...]
            for s, p in some:
                for j in range(2):
                    at = slice(s * row_span + (2 * p + j) * block, s * row_span + (2 * p + j + 1) * block)
                    high_of = rows_high[s][2 * p + j]
                    for h in range(highs):
                        held = high_of == jnp.asarray(h, BF)
                        for f in range(whole // 16):
                            spread[h * field_pad + f * 16 : h * field_pad + (f + 1) * 16, at] = jnp.where(
                                held, up_in[s, p, j * whole + f * 16 : j * whole + (f + 1) * 16], zero)
                        spread[h * field_pad + whole : (h + 1) * field_pad, at] = jnp.where(
                            held, up_in[s, p, 2 * whole :] * side[j], zero)
                at = slice(s * row_span + 2 * p * block, s * row_span + (2 * p + 2) * block)
                total = total + lax.dot_general(spread[:, at], near[:, at], NT, preferred_element_type=F32)
            flux_out[...] = total

        build(0)
        late = min(5, tiles)
        for c in range(late):
            product(c, cells)
            if c + 1 < tiles:
                build(c + 1)
        take_halo(sides, opool, levels_o, cells, neighbours)

        @pl.when(not_last)
        def _():
            for s in range(air_groups):
                code_relay(s).wait_recv()
                code_relay(s).start()

        for c in range(late):
            rim(c)
        order = [(s, p) for p in range(pairs) for s in reversed(range(air_groups))]

        def relays(some):
            @pl.when(not_last)
            def _():
                for s, p in some:
                    relay_copy(s, p).wait_recv()
                    relay_copy(s, p).start()

        for c in range(late, tiles):
            product(c, omat.shape[0])
            if c + 1 < tiles:
                build(c + 1)
        relays(order)
        code()
        for n in range(0, len(order), 2):

            @pl.when(jnp.logical_not(not_last))
            def _():
                for s, p in order[n : n + 2]:
                    relay_copy(s, p).wait_recv()

            collect(order[n : n + 2])
        for s in range(air_groups):
            down_copy(s, mine).wait_send()

        @pl.when(not_last)
        def _():
            for s in range(air_groups):
                code_relay(s).wait_send()
                for p in range(pairs):
                    relay_copy(s, p).wait_send()

        l_air.wait()


def finish(air_groups, a, b, c, flux, force, a_out, b_out, c_out, held, sem):
    is_air = lax.axis_index("grp") < air_groups
    base, field_pad = flux.shape[1], force.shape[1] // 4
    highs = flux.shape[0] // field_pad
    levels = b.shape[2]
    lines = a.shape[2] // 4
    early = [
        pltpu.make_async_copy(a.at[0, 0, pl.ds(i * lines, lines)], a_out.at[0, 0, pl.ds(i * lines, lines)], sem.at[i])
        for i in range(4)
    ]
    early.append(pltpu.make_async_copy(c, c_out, sem.at[4]))
    for x in early:
        x.start()
    steps = 4 if highs % 4 == 0 else 1

    @pl.when(is_air)
    def _():
        whole = []
        for i in range(steps):
            at = slice(i * highs // steps * base, (i + 1) * highs // steps * base)
            whole.append(pltpu.make_async_copy(b.at[0, 0, :, at], b_out.at[0, 0, :, at], sem.at[5 + i]))
            whole[-1].start()
        for x in whole:
            x.wait()

    @pl.when(jnp.logical_not(is_air))
    def _():
        copies = []
        for i in range(steps):
            for h in range(i * highs // steps, (i + 1) * highs // steps):
                at = slice(h * base, (h + 1) * base)
                here = flux[h * field_pad : (h + 1) * field_pad]
                top = here.astype(BF)
                rest = (here - top.astype(F32)).astype(BF)
                three = jnp.concatenate([top, rest, top], axis=0)
                held[0, 0, :, at] = b[0, 0, :, at] + mm(force[:levels, : 3 * field_pad], three)
            at = slice(i * highs // steps * base, (i + 1) * highs // steps * base)
            copies.append(pltpu.make_async_copy(held.at[0, 0, :, at], b_out.at[0, 0, :, at], sem.at[5 + i]))
            copies[-1].start()
        for x in copies:
            x.wait()

    for x in early:
        x.wait()


def solution(mesh):
    groups, devs = mesh.shape["grp"], mesh.shape["dev"]
    in_specs = (
        P("grp", "dev", None, None), P("grp", "dev", None, None), P("grp", "dev", None),
        P("grp", "dev", None), P(), P("grp", "dev", None), P("grp", "dev", None),
        P("grp", "dev", None, None), P("grp", "dev", None, None, None),
        P("grp", "dev", None, None), P("grp", "dev", None, None), P("grp", "dev", None),
        P("grp", "dev", None), P(), P(),
    )
    out_specs = (P("grp", "dev", None, None),) * 3

    def on_device(*args):
        args = list(args)
        args[5] = args[5].reshape(-1, 128)
        args[7] = args[7].transpose(0, 1, 3, 2)
        args[8] = args[8].transpose(0, 1, 3, 2, 4)
        args[10] = args[10].transpose(0, 2, 1, 3)
        args[13] = args[13].T
        air, anbr, asend, amix, fw, counts, mw, owner, recv, sea, onbr, osend, omix, force, ret = args
        levels_a, columns = air.shape[2:]
        levels_o, cells = sea.shape[2:]
        half = asend.shape[2] // 2
        capacity, air_groups, block = recv.shape[2:]
        sea_groups = groups - air_groups
        blocks = owner.shape[3]
        fields, ret_fields = fw.shape[0], ret.shape[0]
        ret_pad = -(-ret_fields // 16) * 16
        field_pad = -(-fields // 16) * 16
        row_count = mw.shape[2]
        pairs = blocks // 2
        pool_a, pool_o = columns + 2 * half, cells + 2 * half
        width = 256
        base, span = base_of(cells), air_groups * capacity * block
        row_span = air_groups * blocks * block
        same = capacity == blocks
        deep = max(
            anbr.shape[2] * (pool_a // base_of(pool_a)),
            onbr.shape[1] * (pool_o // base_of(pool_o)),
        )
        code_rows = -(-blocks // 8) * 8
        V = pltpu.VMEM
        dma = pltpu.SemaphoreType.DMA
        kept = [V(x.shape, x.dtype) for x in (anbr, asend, amix, fw, counts, mw)]
        kept += [pltpu.SMEM(owner.shape, owner.dtype)]
        kept += [V(x.shape, x.dtype) for x in (recv, onbr, osend, omix, force, ret)]
        levels = max(levels_a, levels_o)
        scratch = kept + [
            V((2, levels, half), BF), V((2, levels, half), BF),
            V((2, 2 * fields, half), BF), V((2, 2 * fields, half), BF),
            V((levels_a, pool_a), BF), V((2 * fields, columns), BF), V((levels_o, pool_o), BF), V((max(columns, cells), 2 * half), BF),
            V((pool_a, columns), BF), V((pool_o, cells), BF),
            V((columns, row_count), BF), V((2 * half, row_count), BF), V((fields + 8, row_count), F32),
            V((base, span), BF),
            V((base if not same else 16, row_span if not same else 128), BF),
            V((cells // base * field_pad, row_span), BF),
            V((deep, 16, width), BF),
            V((code_rows, 128), I32), V((air_groups, code_rows, 128), I32),
            V((pairs, 2 * fields, block), BF), V((air_groups, pairs, 2 * fields, block), BF),
            V((air_groups, capacity, ret_pad, block), BF), V((sea_groups, capacity, ret_pad, block), BF),
            V((ret_pad, levels_o), F32),
            V((max(4 * ret_pad, 2 * fields + 16), max(row_count, columns)), BF),
            V((cells // base * ret_pad, base), BF),
            V((4 * field_pad, 128), F32),
            dma((4,)), dma((max(air_groups, sea_groups),)), dma((air_groups, pairs)), pltpu.SemaphoreType.REGULAR,
        ]
        sends = ((9,), (4,), (2 * air_groups,), (air_groups, pairs))
        vmem = pl.BlockSpec(memory_space=pltpu.VMEM)
        outs = (
            jax.ShapeDtypeStruct(air.shape, F32),
            jax.ShapeDtypeStruct(sea.shape, F32),
            jax.ShapeDtypeStruct((1, ret_fields, 1, columns), F32),
        )
        kept_outs = outs + (
            jax.ShapeDtypeStruct((cells // base * field_pad, base), F32),
            jax.ShapeDtypeStruct((128, 4 * field_pad), BF),
        )
        parts = pl.pallas_call(
            functools.partial(kernel, (groups, devs, air_groups, sends)),
            out_shape=kept_outs,
            in_specs=[pl.BlockSpec(memory_space=pltpu.HBM)] * 15,
            out_specs=(vmem,) * 5,
            scratch_shapes=scratch,
            compiler_params=pltpu.CompilerParams(
                collective_id=0, has_side_effects=True, vmem_limit_bytes=48 * 1024 * 1024),
            name="couple",
        )(*[pltpu.with_memory_space_constraint(x, pltpu.HBM) for x in args])
        air_next, sea_next, back = pl.pallas_call(
            functools.partial(finish, air_groups),
            out_shape=outs,
            in_specs=[vmem] * 5,
            out_specs=(pl.BlockSpec(memory_space=pl.ANY),) * 3,
            scratch_shapes=[V(sea.shape, F32), dma((9,))],
            compiler_params=pltpu.CompilerParams(vmem_limit_bytes=4 * 1024 * 1024),
            name="finish",
        )(*parts)
        return air_next, sea_next, back.transpose(0, 2, 1, 3)

    return jax.shard_map(
        on_device, mesh=mesh, in_specs=in_specs, out_specs=out_specs, check_vma=False)
```

```python
import functools

import jax
import jax.numpy as jnp
from jax import lax
from jax.experimental import pallas as pl
from jax.experimental.pallas import tpu as pltpu
from jax.sharding import PartitionSpec as P

EXACT = lax.Precision.HIGHEST
BF = jnp.bfloat16
F32 = jnp.float32
I32 = jnp.int32
NT = (((1,), (1,)), ((), ()))
TN = (((0,), (0,)), ((), ()))


def mm(a, b):
    return jnp.dot(a, b, preferred_element_type=F32)


def two_parts(x):
    rest = x - x.astype(BF).astype(F32)
    return jnp.concatenate([x, rest], axis=0).astype(BF)


def joined(x):
    half = x.shape[0] // 2
    return x[:half] + x[half:]


def low_hot(low, t):
    place = lax.broadcasted_iota(I32, low.shape, 0).astype(F32) + 16.0 * t
    return jnp.where(low == place.astype(BF), jnp.asarray(1, BF), jnp.asarray(0, BF))


def as_rows(idx, rows):
    return jnp.broadcast_to(idx.astype(F32), (rows, idx.shape[1])).astype(BF)


def hot_rows(high, h, rows):
    return jnp.where(as_rows(high, rows) == jnp.asarray(h, BF), jnp.asarray(1, BF), jnp.asarray(0, BF))


def one_hot_matrix(out_ref, idx, base):
    bits = base.bit_length() - 1
    low = as_rows(idx & (base - 1), 16)
    marks = [hot_rows(idx >> bits, h, 16) for h in range(out_ref.shape[0] // base)]
    for t in range(base // 16):
        part = low_hot(low, t)
        for h, mark in enumerate(marks):
            out_ref[h * base + t * 16 : h * base + (t + 1) * 16, :] = part * mark


def couples(highs, neighbours):
    step = 2 if neighbours < 8 else 1
    return [tuple(range(h, min(h + step, highs))) for h in range(0, highs, step)]


def scale_at(position, length, base, neighbours):
    for couple in couples(length // base, neighbours):
        if position // base in couple:
            return 16.0 if len(couple) == 2 and position // base == couple[0] else 1.0


def scaled(x, at, length, base, neighbours):
    return x * jnp.asarray(scale_at(at, length, base, neighbours), BF)


def counts_matrix(out_ref, high_ref, idx_rows, base, at):
    highs = out_ref.shape[0] // base
    bits = base.bit_length() - 1
    lines = couples(highs, len(idx_rows))
    low = [as_rows(i & (base - 1), 16) for i in idx_rows]
    for k, i in enumerate(idx_rows):
        top = as_rows(i >> bits, 16)
        for n, couple in enumerate(lines):
            mark = jnp.where(top == jnp.asarray(couple[-1], BF), jnp.asarray(1, BF), jnp.asarray(0, BF))
            if len(couple) == 2:
                mark = jnp.where(top == jnp.asarray(couple[0], BF), jnp.asarray(1 / 16, BF), mark)
            high_ref[k * len(lines) + n] = mark
    for t in range(base // 16):
        parts = [low_hot(i, t) for i in low]
        for n, couple in enumerate(lines):
            total = parts[0] * high_ref[n]
            for k in range(1, len(parts)):
                total = total + parts[k] * high_ref[k * len(lines) + n]
            if len(couple) == 2:
                whole = (total + jnp.asarray(128, BF)) - jnp.asarray(128, BF)
                out_ref[couple[0] * base + t * 16 : couple[0] * base + (t + 1) * 16, at] = total - whole
                total = whole
            out_ref[couple[-1] * base + t * 16 : couple[-1] * base + (t + 1) * 16, at] = total


def base_of(length):
    return 256 if length % 256 == 0 else 128


def row_columns(counts, rows):
    lines = counts.shape[0]
    wide = jnp.concatenate([counts.astype(F32), jnp.zeros((-lines % 16, 128), F32)], axis=0).astype(BF)
    lines = wide.shape[0]
    i = lax.broadcasted_iota(I32, (128, 128), 0)
    j = lax.broadcasted_iota(I32, (128, 128), 1)
    within = mm(wide, jnp.where(i <= j, 1.0, 0.0).astype(BF))
    i = lax.broadcasted_iota(I32, (lines, lines), 0)
    j = lax.broadcasted_iota(I32, (lines, lines), 1)
    ones = jnp.ones((128, 128), BF)
    before = mm(mm(jnp.where(j < i, 1.0, 0.0).astype(BF), wide).astype(BF), ones)
    upto = mm(mm(jnp.where(j <= i, 1.0, 0.0).astype(BF), wide).astype(BF), ones)
    offsets = within + before
    high = jnp.floor(offsets * (1.0 / 256.0)) * 256.0
    halves = jnp.concatenate([high, offsets - high], axis=0).astype(BF)
    tiles = rows // 128
    at = lax.broadcasted_iota(I32, (lines, rows), 1).astype(F32)
    ends = jnp.concatenate([upto] * tiles, axis=1)
    starts = jnp.concatenate([before] * tiles, axis=1)
    passed = jnp.where(ends <= at, 1.0, 0.0)
    line = jnp.where(starts <= at, 1.0, 0.0) - passed
    line = jnp.concatenate([line, line], axis=0).astype(BF)
    ends_in = lax.dot_general(halves, line, TN, preferred_element_type=F32)
    at = lax.broadcasted_iota(I32, (128, rows), 1).astype(F32)
    inner = jnp.sum(jnp.where(ends_in <= at, 1.0, 0.0), axis=0, keepdims=True)
    return 128.0 * jnp.sum(passed, axis=0, keepdims=True) + inner


def kernel(sizes, *refs):
    pl.run_scoped(
        functools.partial(body, sizes[:3], refs),
        *(pltpu.SemaphoreType.DMA(n) for n in sizes[3]))


def body(
    sizes, refs, load, halo_send, x_send, up_send,
):
    (
        air_hbm, anbr_hbm, asend_hbm, amix_hbm, fw_hbm, counts_hbm, mw_hbm, owner_hbm,
        recv_hbm, sea_hbm, onbr_hbm, osend_hbm, omix_hbm, force_hbm, retw_hbm,
        air_out, sea_out, back_out, flux_out, force_out,
        anbr, asend, amix, fw, counts, mw, owner, recv, onbr, osend, omix, force, retw_in,
        pack, halo, gpack, ghalo, apool, gpool, opool, picker, amat, omat, member, ahead, early, lowmat, lowrow, spread, high,
        codes_out, codes_in, up_out, up_in, down_out, down_in, retw, slab, ret_bf, wide_force,
        halo_recv, x_recv, up_recv, told,
    ) = refs
    groups, devs, air_groups = sizes
    sea_groups = groups - air_groups
    g, d = lax.axis_index("grp"), lax.axis_index("dev")
    lower, upper = lax.rem(d + devs - 1, devs), lax.rem(d + 1, devs)
    is_air = g < air_groups
    mine = jnp.where(is_air, g, g - air_groups)
    half = halo.shape[2]
    capacity, block = recv.shape[2], recv.shape[4]
    span = capacity * block
    levels_a, columns = air_out.shape[2:]
    levels_o, cells = sea_out.shape[2:]
    fields = fw.shape[0]
    ret_fields = retw_in.shape[0]
    ret_pad = retw.shape[0]
    blocks = owner.shape[3]
    row_count = mw.shape[2]
    pairs = blocks // 2
    same = capacity == blocks
    base = lowmat.shape[0]
    bits = base.bit_length() - 1
    highs = cells // base
    field_pad = spread.shape[0] // highs
    width = high.shape[2]

    barrier = pltpu.get_barrier_semaphore()
    pl.semaphore_signal(barrier, inc=1, device_id={"dev": lower})
    pl.semaphore_signal(barrier, inc=1, device_id={"dev": upper})

    def loads(*copies):
        return [pltpu.make_async_copy(a, b, load.at[i]) for i, (a, b) in enumerate(copies)]

    def halos(source, target, levels, first):
        return [
            pltpu.make_async_remote_copy(
                src_ref=source.at[1 - side, :levels], dst_ref=target.at[side, :levels],
                send_sem=halo_send.at[first + side], recv_sem=halo_recv.at[first + side],
                device_id={"dev": upper if side == 0 else lower})
            for side in range(2)
        ]

    def code_copy(s):
        return pltpu.make_async_remote_copy(
            src_ref=codes_out, dst_ref=codes_in.at[s], send_sem=x_send.at[0],
            recv_sem=x_recv.at[s], device_id={"grp": air_groups})

    def code_relay(s):
        return pltpu.make_async_remote_copy(
            src_ref=codes_in.at[s], dst_ref=codes_in.at[s], send_sem=x_send.at[air_groups + s],
            recv_sem=x_recv.at[s], device_id={"grp": g + 1})

    def down_copy(s, o):
        return pltpu.make_async_remote_copy(
            src_ref=down_out.at[s], dst_ref=down_in.at[o], send_sem=x_send.at[s],
            recv_sem=x_recv.at[o], device_id={"grp": s})

    def up_copy(s, p):
        return pltpu.make_async_remote_copy(
            src_ref=up_out.at[p], dst_ref=up_in.at[s, p], send_sem=up_send.at[0, p],
            recv_sem=up_recv.at[s, p], device_id={"grp": air_groups})

    def relay_copy(s, p):
        return pltpu.make_async_remote_copy(
            src_ref=up_in.at[s, p], dst_ref=up_in.at[s, p], send_sem=up_send.at[s, p],
            recv_sem=up_recv.at[s, p], device_id={"grp": g + 1})

    def packed(chosen, to, levels):
        to[0, :levels, :] = chosen[:, :half]
        to[1, :levels, :] = chosen[:, half:]

    def take_halo(copies, pool, levels, length, neighbours):
        for c in copies:
            c.wait()
        for side in range(2):
            at = slice(length + side * half, length + (side + 1) * half)
            pool[:, at] = scaled(halo[side, :levels, :], at.start, pool.shape[1], base_of(pool.shape[1]), neighbours)

    @pl.when(is_air)
    def _():
        pl.semaphore_signal(barrier, inc=1, device_id={"grp": air_groups})
        (l_asend, l_air, l_fw, l_owner, l_counts, l_anbr, l_amix, l_mw, l_sea) = loads(
            (asend_hbm, asend), (air_hbm, air_out), (fw_hbm, fw), (owner_hbm, owner), (counts_hbm, counts),
            (anbr_hbm, anbr), (amix_hbm, amix), (mw_hbm, mw), (sea_hbm, sea_out))
        for c in (l_asend, l_air, l_fw, l_anbr, l_counts, l_amix, l_mw, l_owner):
            c.start()
        neighbours = anbr.shape[2]
        excess = row_count - columns
        tile = 256

        l_asend.wait()
        base_a = base_of(amat.shape[0])
        one_hot_matrix(picker.at[:columns], asend[0], base_of(columns))
        l_fw.wait()
        weight = two_parts(fw[...])
        l_air.wait()
        state = air_out[0, 0]
        top = state.astype(BF)
        own = joined(mm(weight, top) + mm(weight, (state - top.astype(F32)).astype(BF)))
        own_parts = two_parts(own)
        packed(mm(own_parts, picker[:columns]).astype(BF), gpack, 2 * fields)
        pl.semaphore_wait(barrier, 3)
        near_sides = halos(gpack, ghalo, 2 * fields, 2)
        for c in near_sides:
            c.start()
        l_owner.wait()
        owners = [owner[0, 0, 0, b] for b in range(blocks)]
        slots = []
        for b in range(blocks):
            s = jnp.int32(b if same else 0)
            if not same:
                for e in range(b):
                    s = s + jnp.where(owners[e] == owners[b], 1, 0)
            slots.append(s)
        for b in range(blocks):
            codes_out[b : b + 1, :] = jnp.full((1, 128), owners[b] * capacity + slots[b], I32)
        if codes_out.shape[0] > blocks:
            codes_out[blocks:, :] = jnp.full((codes_out.shape[0] - blocks, 128), -1, I32)
        code_copy(mine).start()
        l_sea.start()

        l_anbr.wait()
        l_amix.wait()
        l_mw.wait()
        for c in range(columns // width):
            at = slice(c * width, (c + 1) * width)
            counts_matrix(amat, high, [anbr[0, 0, k : k + 1, at] for k in range(neighbours)], base_a, at)
        for h in range(columns // base_a):
            at = slice(h * base_a, (h + 1) * base_a)
            apool[:, at] = scaled(top[:, at], at.start, amat.shape[0], base_a, neighbours)
            gpool[:, at] = scaled(own_parts[:, at], at.start, amat.shape[0], base_a, neighbours)
        for c in range(columns // tile):
            at = slice(c * tile, (c + 1) * tile)
            mean = joined(mm(gpool[...], amat[:columns, at])) * (1.0 / neighbours)
            here, mix = own[:, at], amix[0, :, at]
            flux = here + mix * (mean - here)
            slab[: 2 * fields, at] = two_parts(flux)
            slab[2 * fields : 2 * fields + 16, at] = two_parts(jnp.broadcast_to(mix, (8, tile)))
        l_counts.wait()
        column = row_columns(counts[...], row_count).astype(I32)
        low, high_of = column & (tile - 1), column >> (tile.bit_length() - 1)
        low_rows = as_rows(low, 16)

        def reach(p):
            first = max(0, p * tile - excess) // tile
            last = min(columns - 1, p * tile + tile - 1) // tile
            return range(first, last + 1)

        for p in range(row_count // tile):
            at = slice(p * tile, (p + 1) * tile)
            marks = [hot_rows(high_of[:, at], h, 16) for h in reach(p)]
            for t in range(tile // 16):
                part = low_hot(low_rows[:, at], t)
                for i, h in enumerate(reach(p)):
                    member[h * tile + t * 16 : h * tile + (t + 1) * 16, at] = part * marks[i]

        for p in range(row_count // tile):
            at = slice(p * tile, (p + 1) * tile)
            ks = reach(p)
            ks = slice(ks[0] * tile, (ks[-1] + 1) * tile)
            both = mm(jnp.concatenate([slab[: 2 * fields + 16, ks], amat[columns:, ks]], axis=0), member[ks, at])
            share = mw[0, :, at]
            mix = joined(both[2 * fields : 2 * fields + 16])[:1]
            early[:fields, at] = joined(both[: 2 * fields]) * share
            early[fields : fields + 8, at] = jnp.broadcast_to(share * mix * (1.0 / neighbours), (8, tile))
            ahead[:, at] = both[2 * fields + 16 :].astype(BF)
        for c in near_sides:
            c.wait()
        far = jnp.concatenate([
            scaled(ghalo[side], columns + side * half, amat.shape[0], base_a, neighbours) for side in range(2)], axis=1)
        for p in range(row_count // tile):
            at = slice(p * tile, (p + 1) * tile)
            values = early[:fields, at] + early[fields : fields + 1, at] * joined(mm(far, ahead[:, at]))
            per = tile // block
            for q in range(per // 2):
                b = slice(2 * q * block, (2 * q + 1) * block), slice((2 * q + 1) * block, (2 * q + 2) * block)
                whole = fields - fields % 16
                up_out[p * (per // 2) + q] = jnp.concatenate(
                    [values[f, at] for f in (slice(whole), slice(whole, None)) for at in b], axis=0).astype(BF)
                up_copy(mine, p * (per // 2) + q).start()
        packed(mm(air_out[0, 0].astype(BF), picker[:columns]).astype(BF), pack, levels_a)
        sides = halos(pack, halo, levels_a, 0)
        for c in sides:
            c.start()
        take_halo(sides, apool, levels_a, columns, neighbours)
        for c in range(columns // width):
            at = slice(c * width, (c + 1) * width)
            mean = mm(apool[...], amat[:, at]) * (1.0 / neighbours)
            here = air_out[0, 0, :, at]
            air_out[0, 0, :, at] = here + amix[0, :, at] * (mean - here)
        for o in range(sea_groups):
            down_copy(0, o).wait_recv()
        for b in range(blocks):
            at = slice(b * block, (b + 1) * block)
            share = jnp.broadcast_to(mw[0, :, at], (ret_pad, block))
            value = down_in[owners[b], slots[b]].astype(F32) * share
            slab[: 2 * ret_pad, at] = two_parts(value)
            slab[2 * ret_pad : 4 * ret_pad, at] = two_parts(share)
        for c in range(columns // tile):
            at = slice(c * tile, (c + 1) * tile)
            rs = slice(c * tile, min(row_count, (c + 1) * tile + excess))
            sums = lax.dot_general(slab[: 4 * ret_pad, rs], member[at, rs], NT, preferred_element_type=F32)
            ratio = joined(sums[: 2 * ret_pad]) / joined(sums[2 * ret_pad :])
            for f in range(ret_fields):
                back_out[0, f, :, at] = ratio[f : f + 1]
        code_copy(mine).wait_send()
        for p in range(pairs):
            up_copy(mine, p).wait_send()
        l_sea.wait()

    @pl.when(jnp.logical_not(is_air))
    def _():
        not_first, not_last = mine > 0, mine < sea_groups - 1

        @pl.when(not_first)
        def _():
            pl.semaphore_signal(barrier, inc=1, device_id={"grp": g - 1})

        @pl.when(jnp.logical_not(not_first))
        def _():
            for s in range(air_groups):
                pl.semaphore_signal(barrier, inc=1, device_id={"grp": s})

        @pl.when(not_last)
        def _():
            pl.semaphore_signal(barrier, inc=1, device_id={"grp": g + 1})

        (l_osend, l_sea, l_retw, l_recv, l_onbr, l_omix, l_force, l_air) = loads(
            (osend_hbm, osend), (sea_hbm, sea_out), (retw_hbm, retw_in), (recv_hbm, recv), (onbr_hbm, onbr),
            (omix_hbm, omix), (force_hbm, force), (air_hbm, air_out))
        for c in (l_osend, l_sea, l_retw, l_recv, l_onbr, l_omix, l_force):
            c.start()
        neighbours = onbr.shape[1]
        l_osend.wait()
        one_hot_matrix(picker.at[:cells], osend[0], base)
        base_p = base_of(omat.shape[0])
        l_sea.wait()
        top = sea_out[0, 0].astype(BF)
        packed(mm(top, picker[:cells]).astype(BF), pack, levels_o)
        links = jnp.where(not_first, 1, air_groups) + jnp.where(not_last, 1, 0)
        pl.semaphore_wait(barrier, 2 + links)
        sides = halos(pack, halo, levels_o, 0)
        for c in sides:
            c.start()

        @pl.when(not_first)
        def _():
            pl.semaphore_wait(told, 1)

        @pl.when(not_last)
        def _():
            pl.semaphore_signal(told, inc=1, device_id={"grp": g + 1})

        l_air.start()
        l_retw.wait()
        l_recv.wait()
        l_onbr.wait()
        l_omix.wait()
        l_force.wait()
        retw[...] = jnp.zeros(retw.shape, F32)
        retw[:ret_fields] = retw_in[...]
        weight = two_parts(retw[...])
        state = sea_out[0, 0]
        top = state.astype(BF)
        rest = (state - top.astype(F32)).astype(BF)
        for h in range(cells // base_p):
            at = slice(h * base_p, (h + 1) * base_p)
            opool[:, at] = scaled(top[:, at], at.start, omat.shape[0], base_p, neighbours)
        returned = joined(mm(weight, top) + mm(weight, rest)).astype(BF)
        for h in range(highs):
            ret_bf[h * ret_pad : (h + 1) * ret_pad] = returned[:, h * base : (h + 1) * base]

        def slot_ids(s):
            return jnp.concatenate([recv[0, 0, k, s : s + 1, :] for k in range(capacity)], axis=1)

        for s in range(air_groups):
            idx = slot_ids(s)
            at = slice(s * span, (s + 1) * span)
            low = as_rows(idx & (base - 1), 16)
            for t in range(base // 16):
                lowmat[t * 16 : (t + 1) * 16, at] = low_hot(low, t)
            found = mm(ret_bf[...], lowmat[:, at])
            high_of = jnp.broadcast_to(idx >> bits, (ret_pad, span))
            looked = jnp.zeros((ret_pad, span), F32)
            for h in range(highs):
                looked = jnp.where(high_of == h, found[h * ret_pad : (h + 1) * ret_pad], looked)
            for k in range(capacity):
                down_out[s, k] = looked[:, k * block : (k + 1) * block].astype(BF)
            down_copy(s, mine).start()
        wide_force[...] = jnp.zeros(wide_force.shape, F32)
        strong = force[...]
        for i, part in enumerate((strong, strong, strong - strong.astype(BF).astype(F32))):
            wide_force[i * field_pad : i * field_pad + fields, :levels_o] = part
            wide_force[i * field_pad + fields : (i + 1) * field_pad, :levels_o] = part[fields - fields % 16 :]
        force_out[...] = wide_force[...].T.astype(BF)
        flux_out[...] = jnp.zeros(flux_out.shape, F32)
        back_out[...] = jnp.zeros(back_out.shape, F32)
        tiles = cells // width
        row_span = blocks * block
        near = lowmat if same else lowrow

        def build(c):
            at = slice(c * width, (c + 1) * width)
            counts_matrix(omat, high, [onbr[0, k, :, at] for k in range(neighbours)], base_p, at)

        def product(c, depth):
            at = slice(c * width, (c + 1) * width)
            mean = mm(opool[:, :depth], omat[:depth, at]) * (1.0 / neighbours)
            here = sea_out[0, 0, :, at]
            sea_out[0, 0, :, at] = here + omix[0, :, at] * (mean - here)

        def rim(c):
            at = slice(c * width, (c + 1) * width)
            mean = mm(opool[:, cells:], omat[cells:, at]) * (1.0 / neighbours)
            sea_out[0, 0, :, at] += omix[0, :, at] * mean

        rows_high = []
        whole = fields - fields % 16
        zero = jnp.asarray(0, BF)
        lines = lax.broadcasted_iota(I32, (16, block), 0)
        side = [jnp.where((lines >= 8 * j) & (lines < 8 * j + 8), 1.0, 0.0).astype(BF) for j in range(2)]

        def code():
            @pl.when(jnp.logical_not(not_last))
            def _():
                for s in range(air_groups):
                    code_relay(s).wait_recv()

            for s in range(air_groups):
                place = codes_in[s] - mine * capacity
                ids = []
                for b in range(blocks):
                    here = place[b : b + 1]
                    held = (here >= 0) & (here < capacity)
                    if same:
                        cell = recv[0, 0, b, s : s + 1, :]
                    else:
                        cell = jnp.zeros((1, block), I32)
                        for k in range(capacity):
                            cell = jnp.where(here == k, recv[0, 0, k, s : s + 1, :], cell)
                    ids.append(jnp.where(held, cell, -1))
                rows_high.append([as_rows(i >> bits, 16) for i in ids])
                if not same:
                    low = as_rows(jnp.concatenate(ids, axis=1) & (base - 1), 16)
                    for t in range(base // 16):
                        lowrow[t * 16 : (t + 1) * 16, s * row_span : (s + 1) * row_span] = low_hot(low, t)

        def collect(some):
            total = flux_out[...]
            for s, p in some:
                for j in range(2):
                    at = slice(s * row_span + (2 * p + j) * block, s * row_span + (2 * p + j + 1) * block)
                    high_of = rows_high[s][2 * p + j]
                    for h in range(highs):
                        held = high_of == jnp.asarray(h, BF)
                        for f in range(whole // 16):
                            spread[h * field_pad + f * 16 : h * field_pad + (f + 1) * 16, at] = jnp.where(
                                held, up_in[s, p, j * whole + f * 16 : j * whole + (f + 1) * 16], zero)
                        spread[h * field_pad + whole : (h + 1) * field_pad, at] = jnp.where(
                            held, up_in[s, p, 2 * whole :] * side[j], zero)
                at = slice(s * row_span + 2 * p * block, s * row_span + (2 * p + 2) * block)
                total = total + lax.dot_general(spread[:, at], near[:, at], NT, preferred_element_type=F32)
            flux_out[...] = total

        build(0)
        late = min(5, tiles)
        for c in range(late):
            product(c, cells)
            if c + 1 < tiles:
                build(c + 1)
        take_halo(sides, opool, levels_o, cells, neighbours)

        @pl.when(not_last)
        def _():
            for s in range(air_groups):
                code_relay(s).wait_recv()
                code_relay(s).start()

        for c in range(late):
            rim(c)
        order = [(s, p) for p in range(pairs) for s in reversed(range(air_groups))]

        def relays(some):
            @pl.when(not_last)
            def _():
                for s, p in some:
                    relay_copy(s, p).wait_recv()
                    relay_copy(s, p).start()

        for c in range(late, tiles):
            product(c, omat.shape[0])
            if c + 1 < tiles:
                build(c + 1)
        relays(order)
        code()
        groups_of = [order[n : n + 2] for n in range(0, len(order) - 2, 2)] + [[x] for x in order[-2:]]
        for some in groups_of:

            @pl.when(jnp.logical_not(not_last))
            def _():
                for s, p in some:
                    relay_copy(s, p).wait_recv()

            collect(some)
        for s in range(air_groups):
            down_copy(s, mine).wait_send()

        @pl.when(not_last)
        def _():
            for s in range(air_groups):
                code_relay(s).wait_send()
                for p in range(pairs):
                    relay_copy(s, p).wait_send()

        l_air.wait()


def finish(air_groups, a, b, c, flux, force, a_out, b_out, c_out, held, sem):
    is_air = lax.axis_index("grp") < air_groups
    base, field_pad = flux.shape[1], force.shape[1] // 4
    highs = flux.shape[0] // field_pad
    levels = b.shape[2]
    lines = a.shape[2] // 4
    early = [
        pltpu.make_async_copy(a.at[0, 0, pl.ds(i * lines, lines)], a_out.at[0, 0, pl.ds(i * lines, lines)], sem.at[i])
        for i in range(4)
    ]
    early.append(pltpu.make_async_copy(c, c_out, sem.at[4]))
    for x in early:
        x.start()
    steps = 4 if highs % 4 == 0 else 1

    @pl.when(is_air)
    def _():
        whole = []
        for i in range(steps):
            at = slice(i * highs // steps * base, (i + 1) * highs // steps * base)
            whole.append(pltpu.make_async_copy(b.at[0, 0, :, at], b_out.at[0, 0, :, at], sem.at[5 + i]))
            whole[-1].start()
        for x in whole:
            x.wait()

    @pl.when(jnp.logical_not(is_air))
    def _():
        copies = []
        for i in range(steps):
            for h in range(i * highs // steps, (i + 1) * highs // steps):
                at = slice(h * base, (h + 1) * base)
                here = flux[h * field_pad : (h + 1) * field_pad]
                top = here.astype(BF)
                rest = (here - top.astype(F32)).astype(BF)
                three = jnp.concatenate([top, rest, top], axis=0)
                held[0, 0, :, at] = b[0, 0, :, at] + mm(force[:levels, : 3 * field_pad], three)
            at = slice(i * highs // steps * base, (i + 1) * highs // steps * base)
            copies.append(pltpu.make_async_copy(held.at[0, 0, :, at], b_out.at[0, 0, :, at], sem.at[5 + i]))
            copies[-1].start()
        for x in copies:
            x.wait()

    for x in early:
        x.wait()


def solution(mesh):
    groups, devs = mesh.shape["grp"], mesh.shape["dev"]
    in_specs = (
        P("grp", "dev", None, None), P("grp", "dev", None, None), P("grp", "dev", None),
        P("grp", "dev", None), P(), P("grp", "dev", None), P("grp", "dev", None),
        P("grp", "dev", None, None), P("grp", "dev", None, None, None),
        P("grp", "dev", None, None), P("grp", "dev", None, None), P("grp", "dev", None),
        P("grp", "dev", None), P(), P(),
    )
    out_specs = (P("grp", "dev", None, None),) * 3

    def on_device(*args):
        args = list(args)
        args[5] = args[5].reshape(-1, 128)
        args[7] = args[7].transpose(0, 1, 3, 2)
        args[8] = args[8].transpose(0, 1, 3, 2, 4)
        args[10] = args[10].transpose(0, 2, 1, 3)
        args[13] = args[13].T
        air, anbr, asend, amix, fw, counts, mw, owner, recv, sea, onbr, osend, omix, force, ret = args
        levels_a, columns = air.shape[2:]
        levels_o, cells = sea.shape[2:]
        half = asend.shape[2] // 2
        capacity, air_groups, block = recv.shape[2:]
        sea_groups = groups - air_groups
        blocks = owner.shape[3]
        fields, ret_fields = fw.shape[0], ret.shape[0]
        ret_pad = -(-ret_fields // 16) * 16
        field_pad = -(-fields // 16) * 16
        row_count = mw.shape[2]
        pairs = blocks // 2
        pool_a, pool_o = columns + 2 * half, cells + 2 * half
        width = 256
        base, span = base_of(cells), air_groups * capacity * block
        row_span = air_groups * blocks * block
        same = capacity == blocks
        deep = max(
            anbr.shape[2] * (pool_a // base_of(pool_a)),
            onbr.shape[1] * (pool_o // base_of(pool_o)),
        )
        code_rows = -(-blocks // 8) * 8
        V = pltpu.VMEM
        dma = pltpu.SemaphoreType.DMA
        kept = [V(x.shape, x.dtype) for x in (anbr, asend, amix, fw, counts, mw)]
        kept += [pltpu.SMEM(owner.shape, owner.dtype)]
        kept += [V(x.shape, x.dtype) for x in (recv, onbr, osend, omix, force, ret)]
        levels = max(levels_a, levels_o)
        scratch = kept + [
            V((2, levels, half), BF), V((2, levels, half), BF),
            V((2, 2 * fields, half), BF), V((2, 2 * fields, half), BF),
            V((levels_a, pool_a), BF), V((2 * fields, columns), BF), V((levels_o, pool_o), BF), V((max(columns, cells), 2 * half), BF),
            V((pool_a, columns), BF), V((pool_o, cells), BF),
            V((columns, row_count), BF), V((2 * half, row_count), BF), V((fields + 8, row_count), F32),
            V((base, span), BF),
            V((base if not same else 16, row_span if not same else 128), BF),
            V((cells // base * field_pad, row_span), BF),
            V((deep, 16, width), BF),
            V((code_rows, 128), I32), V((air_groups, code_rows, 128), I32),
            V((pairs, 2 * fields, block), BF), V((air_groups, pairs, 2 * fields, block), BF),
            V((air_groups, capacity, ret_pad, block), BF), V((sea_groups, capacity, ret_pad, block), BF),
            V((ret_pad, levels_o), F32),
            V((max(4 * ret_pad, 2 * fields + 16), max(row_count, columns)), BF),
            V((cells // base * ret_pad, base), BF),
            V((4 * field_pad, 128), F32),
            dma((4,)), dma((max(air_groups, sea_groups),)), dma((air_groups, pairs)), pltpu.SemaphoreType.REGULAR,
        ]
        sends = ((9,), (4,), (2 * air_groups,), (air_groups, pairs))
        vmem = pl.BlockSpec(memory_space=pltpu.VMEM)
        outs = (
            jax.ShapeDtypeStruct(air.shape, F32),
            jax.ShapeDtypeStruct(sea.shape, F32),
            jax.ShapeDtypeStruct((1, ret_fields, 1, columns), F32),
        )
        kept_outs = outs + (
            jax.ShapeDtypeStruct((cells // base * field_pad, base), F32),
            jax.ShapeDtypeStruct((128, 4 * field_pad), BF),
        )
        parts = pl.pallas_call(
            functools.partial(kernel, (groups, devs, air_groups, sends)),
            out_shape=kept_outs,
            in_specs=[pl.BlockSpec(memory_space=pltpu.HBM)] * 15,
            out_specs=(vmem,) * 5,
            scratch_shapes=scratch,
            compiler_params=pltpu.CompilerParams(
                collective_id=0, has_side_effects=True, vmem_limit_bytes=48 * 1024 * 1024),
            name="couple",
        )(*[pltpu.with_memory_space_constraint(x, pltpu.HBM) for x in args])
        air_next, sea_next, back = pl.pallas_call(
            functools.partial(finish, air_groups),
            out_shape=outs,
            in_specs=[vmem] * 5,
            out_specs=(pl.BlockSpec(memory_space=pl.ANY),) * 3,
            scratch_shapes=[V(sea.shape, F32), dma((9,))],
            compiler_params=pltpu.CompilerParams(vmem_limit_bytes=4 * 1024 * 1024),
            name="finish",
        )(*parts)
        return air_next, sea_next, back.transpose(0, 2, 1, 3)

    return jax.shard_map(
        on_device, mesh=mesh, in_specs=in_specs, out_specs=out_specs, check_vma=False)
```
